256 devices in a mesh: dp: 64 (over z_lo, x, y), rep: 4 (over z_hi, core).
Axes of the slice: x: 4, y: 4, z: 8 (z_hi: 2, z_lo: 4; z = z_hi * 4 + z_lo), core: 2. Of those that a mesh axis runs over, the one named last changes fastest.
Arguments:
- encoder_out: bfloat16 [1024, 32, 512], P(('dp', 'rep')), may hold values from -6 to 6
- predictor_out: bfloat16 [1024, 17, 512], P(('dp', 'rep')), may hold values from -6 to 6
- w_encoder: bfloat16 [512, 512], replicated, may hold values from -0.25 to 0.25
- w_predictor: bfloat16 [512, 512], replicated, may hold values from -0.25 to 0.25
- w_joint: bfloat16 [512, 500], replicated, may hold values from -1.296875 to 1.296875
- joint_bias: float32 [500], replicated, may hold values from -8 to 150
- labels: int32 [1024, 16], P(('dp', 'rep')), may hold values from 1 to 499
- frame_lens: int32 [1024], P(('dp', 'rep')), may hold values from 16 to 32, as said below
- label_lens: int32 [1024], P(('dp', 'rep')), may hold values from 1 to 16, as said below
- prune_starts: int32 [1024, 32], P(('dp', 'rep')), may hold values from 0 to 12, as said below
Outputs:
- grad_encoder: float32 [512, 512], replicated
- grad_predictor: float32 [512, 512], replicated
- grad_joint: float32 [512, 500], replicated
- grad_bias: float32 [500], replicated
- loss_mean: float32 [], replicated
The draws below stay inside these ranges and needn't reach their ends.
Inputs may be any that keep to these rules, and one draw needn't show every extreme that they name: `frame_lens`: utterance 0 has 32 frames. `label_lens`: utterance 1 has 16 labels. prune_starts[b,0] = 0; from frame frame_lens[b]-1 on, the start equals max(label_lens[b] - 4, 0), and no start exceeds that value; the starts of consecutive frames differ by at most 3.
All inputs are finite; a program needn't handle non-finite values.
Results may differ from the reference program's by a relative error of at most 0.0059.
Values sent between devices are 32-bit elements; how exact they have to be, the bound alone decides.
No kernel may reach another device: no remote copies, remote signals or barrier semaphores. Data moves between devices by JAX's collectives and lax.ppermute only.
A program may use at most 64 MiB of HBM per device.

```python
import jax
import jax.numpy as jnp
from jax import lax

E = 512
P_SIZE = 512
J = 512
V = 500
S = 5
B_DEV = 4
T_SIZE = 32
U = 16
BATCH = 1024


def utterance_draw(key):
    frame_key = jax.random.fold_in(key, 11)
    label_key = jax.random.fold_in(key, 13)
    jitter_key = jax.random.fold_in(key, 17)
    frame_lens = jax.random.randint(frame_key, (BATCH,), T_SIZE // 2, T_SIZE + 1).at[0].set(T_SIZE)
    label_lens = jax.random.randint(label_key, (BATCH,), 1, U + 1).at[1].set(U)
    upper = jnp.maximum(label_lens + 1 - S, 0)
    frame_index = jnp.arange(T_SIZE, dtype=jnp.int32)[None, :]
    clipped = jnp.minimum(frame_index, frame_lens[:, None] - 1)
    ideal = clipped * upper[:, None] // jnp.maximum(frame_lens[:, None] - 1, 1)
    jitter = jax.random.randint(jitter_key, (BATCH, T_SIZE), -1, 2)
    starts = jnp.clip(ideal + jitter, 0, upper[:, None])
    starts = jnp.where(frame_index == 0, 0, starts)
    starts = jnp.where(frame_index >= frame_lens[:, None] - 1, upper[:, None], starts)
    return (frame_lens.astype(jnp.int32), label_lens.astype(jnp.int32), starts.astype(jnp.int32))


def draw_frame_lens(key, part):
    return utterance_draw(key)[0]


def draw_label_lens(key, part):
    return utterance_draw(key)[1]


def draw_prune_starts(key, part):
    return utterance_draw(key)[2]


def draw_joint_bias(key, part):
    values = jnp.clip(2.0 * jax.random.normal(jax.random.fold_in(key, 31), (V,), jnp.float32), -8.0, 8.0)
    return values


def touch_ends(values, own_key, smallest, top_value):
    longest = values.shape.index(max(values.shape))
    spots = []
    for shift in (0, 1):
        where = [jax.random.randint(jax.random.fold_in(own_key, axis), (), 0, length) for axis, length in enumerate(values.shape)]
        where[longest] = (where[longest] + shift) % values.shape[longest]
        spots.append(tuple(where))
    return values.at[spots[0]].set(smallest).at[spots[1]].set(top_value)


def level_of(key, shape, cuts, smallest, top_value):
    level = 1.0
    for axis_at, blocks in cuts:
        draws = jax.random.uniform(jax.random.fold_in(jax.random.fold_in(key, 6), axis_at), (blocks,), jnp.float32, smallest / len(cuts), top_value / len(cuts))
        level = level * jnp.repeat(jnp.exp(draws), shape[axis_at] // blocks).reshape((-1,) + (1,) * (len(shape) - 1 - axis_at))
    return level


def scatter_about(stream_key, dims, deviation, bound, split=(), kind=jnp.bfloat16):
    level = level_of(stream_key, dims, split, -0.22, 0.18) if split else 1.0
    values = jax.random.normal(stream_key, dims, jnp.float32) * deviation * level
    return jnp.minimum(jnp.maximum(values, -bound), bound).astype(kind)


def setup_inputs(seed: int = 0) -> dict:
    key_list = jax.random.split(jax.random.key(seed), 11)
    encoder_out = scatter_about(key_list[0], (BATCH, T_SIZE, E), 1.0, 6.0, ((0, 256),))
    predictor_out = scatter_about(key_list[1], (BATCH, U + 1, P_SIZE), 1.0, 6.0, ((0, 256),))
    w_encoder = scatter_about(key_list[2], (E, J), E ** -0.5, 0.25)
    w_predictor = scatter_about(key_list[3], (P_SIZE, J), P_SIZE ** -0.5, 0.25)
    w_joint = scatter_about(key_list[4], (J, V), 0.22, 1.296875)
    joint_bias = draw_joint_bias(jax.random.fold_in(key_list[10], 71), 0)
    labels = touch_ends(jax.random.randint(key_list[6], (BATCH, U), 1, V), jax.random.fold_in(key_list[6], 1), 1, V - 1).astype(jnp.int32)
    frame_lens = draw_frame_lens(jax.random.fold_in(key_list[10], 71), 0)
    label_lens = draw_label_lens(jax.random.fold_in(key_list[10], 71), 0)
    prune_starts = draw_prune_starts(jax.random.fold_in(key_list[10], 71), 0)
    return dict(encoder_out=encoder_out, predictor_out=predictor_out, w_encoder=w_encoder, w_predictor=w_predictor, w_joint=w_joint, joint_bias=joint_bias, labels=labels, frame_lens=frame_lens, label_lens=label_lens, prune_starts=prune_starts)


NEG_FILL = -10000.0

def within_frame(entering, emission_now):
    columns = [entering[:, 0]]
    for offset in range(1, entering.shape[1]):
        columns.append(jnp.logaddexp(entering[:, offset], columns[-1] + emission_now[:, offset - 1]))
    return jnp.stack(columns, axis=1)

def lattice(blank_lp, emission, prune_starts, frame_lens, label_lens):
    batches, frames, band = blank_lp.shape
    offsets = jnp.arange(band, dtype=jnp.int32)
    opening = jnp.where(offsets == 0, 0.0, NEG_FILL).astype(blank_lp.dtype)
    forward = within_frame(jnp.broadcast_to(opening, (batches, band)), emission[:, 0])
    shifts = prune_starts[:, 1:] - prune_starts[:, :-1]

    def advance(forward, inputs):
        frame_index, blank_prev, shift_now, emission_now = inputs
        source = offsets[None, :] + shift_now[:, None]
        inside = (source >= 0) & (source < band)
        picked = jnp.take_along_axis(forward + blank_prev, jnp.clip(source, 0, band - 1), axis=1)
        entering = jnp.where(inside, picked, NEG_FILL)
        updated = within_frame(entering, emission_now)
        return (jnp.where((frame_index < frame_lens)[:, None], updated, forward), None)
    inputs = (jnp.arange(1, frames, dtype=jnp.int32), jnp.swapaxes(blank_lp[:, :-1], 0, 1), jnp.swapaxes(shifts, 0, 1), jnp.swapaxes(emission[:, 1:], 0, 1))
    forward, _ = lax.scan(advance, forward, inputs)
    last_frame = (frame_lens - 1).astype(jnp.int32)
    last_start = jnp.take_along_axis(prune_starts, last_frame[:, None], axis=1)[:, 0]
    final_pos = (label_lens - last_start).astype(jnp.int32)
    end_row = jnp.take_along_axis(blank_lp, last_frame[:, None, None], axis=1)[:, 0]
    end_blank = jnp.take_along_axis(end_row, final_pos[:, None], axis=1)[:, 0]
    end_forward = jnp.take_along_axis(forward, final_pos[:, None], axis=1)[:, 0]
    return end_forward + end_blank

def frame_loss(logits, labels, prune_starts, frame_lens, label_lens):
    batches, frames, band, vocab = logits.shape
    positions = prune_starts[:, :, None] + jnp.arange(band, dtype=jnp.int32)
    log_probs = jax.nn.log_softmax(logits, axis=-1)
    label_slots = labels.shape[1]
    next_label = jnp.take_along_axis(labels, jnp.minimum(positions, label_slots - 1).reshape(batches, -1), axis=1)
    next_label = next_label.reshape(positions.shape)
    emission = jnp.take_along_axis(log_probs, next_label[..., None], axis=-1)[..., 0]
    emission = jnp.where(positions < label_lens[:, None, None], emission, NEG_FILL)
    blank_lp = jnp.where(positions <= label_lens[:, None, None], log_probs[..., 0], NEG_FILL)
    likelihood = lattice(blank_lp, emission, prune_starts, frame_lens, label_lens)
    return jnp.sum(-likelihood / frame_lens.astype(jnp.float32))

def block_terms(encoder_out, predictor_out, w_encoder, w_predictor, w_joint, joint_bias, labels, frame_lens, label_lens, prune_starts):
    batches, frames, enc_width = encoder_out.shape
    row_count, pred_width = (predictor_out.shape[1], predictor_out.shape[2])
    joint_width = w_encoder.shape[1]
    vocab = w_joint.shape[1]
    enc_proj = jnp.dot(encoder_out.reshape(-1, enc_width), w_encoder, preferred_element_type=jnp.float32)
    enc_proj = enc_proj.astype(jnp.bfloat16).reshape(batches, frames, joint_width)
    pred_proj = jnp.dot(predictor_out.reshape(-1, pred_width), w_predictor, preferred_element_type=jnp.float32)
    pred_proj = pred_proj.astype(jnp.bfloat16).reshape(batches, row_count, joint_width)
    positions = prune_starts[:, :, None] + jnp.arange(S, dtype=jnp.int32)
    flat_pos = positions.reshape(batches, frames * S)
    picked = jnp.take_along_axis(pred_proj, flat_pos[:, :, None], axis=1).reshape(batches, frames, S, joint_width)
    active = jnp.tanh(enc_proj[:, :, None, :].astype(jnp.float32) + picked.astype(jnp.float32))
    active_flat = active.reshape(-1, joint_width)
    hidden = active_flat.astype(jnp.bfloat16)
    logits = (jnp.dot(hidden, w_joint, preferred_element_type=jnp.float32) + joint_bias).reshape(batches, frames, S, vocab)
    loss_sum, pullback = jax.vjp(lambda scores: frame_loss(scores, labels, prune_starts, frame_lens, label_lens), logits)
    grad_logits, = pullback(jnp.ones((), jnp.float32))
    grad_flat = grad_logits.reshape(-1, vocab)
    grad_low = grad_flat.astype(jnp.bfloat16)
    grad_joint = lax.dot_general(hidden, grad_low, (((0,), (0,)), ((), ())), preferred_element_type=jnp.float32)
    grad_bias = lax.optimization_barrier(jnp.sum(grad_flat, axis=0))
    grad_hidden = lax.dot_general(grad_low, w_joint, (((1,), (1,)), ((), ())), preferred_element_type=jnp.float32)
    grad_pre = (grad_hidden * (1.0 - active_flat * active_flat)).reshape(batches, frames, S, joint_width)
    grad_enc_proj = lax.optimization_barrier(jnp.sum(grad_pre, axis=2)).astype(jnp.bfloat16).reshape(-1, joint_width)
    grad_pre_low = grad_pre.astype(jnp.bfloat16).reshape(batches, frames * S, joint_width)
    placing = (flat_pos[:, :, None] == jnp.arange(row_count, dtype=jnp.int32)).astype(jnp.float32)
    grad_pred_proj = jnp.einsum('bnu,bnj->buj', placing, grad_pre_low.astype(jnp.float32)).astype(jnp.bfloat16)
    grad_encoder = lax.dot_general(encoder_out.reshape(-1, enc_width), grad_enc_proj, (((0,), (0,)), ((), ())), preferred_element_type=jnp.float32)
    grad_predictor = lax.dot_general(predictor_out.reshape(-1, pred_width), grad_pred_proj.reshape(-1, joint_width), (((0,), (0,)), ((), ())), preferred_element_type=jnp.float32)
    return (grad_encoder, grad_predictor, grad_joint, grad_bias, loss_sum)

def reference(encoder_out, predictor_out, w_encoder, w_predictor, w_joint, joint_bias, labels, frame_lens, label_lens, prune_starts):
    groups = BATCH // B_DEV

    def grouped(array):
        return array.reshape((groups, B_DEV) + array.shape[1:])

    def accumulate(totals, pieces):
        block_sums = block_terms(pieces[0], pieces[1], w_encoder, w_predictor, w_joint, joint_bias, pieces[2], pieces[3], pieces[4], pieces[5])
        return (tuple((total + piece for total, piece in zip(totals, block_sums))), None)
    initial = (jnp.zeros(w_encoder.shape, jnp.float32), jnp.zeros(w_predictor.shape, jnp.float32), jnp.zeros(w_joint.shape, jnp.float32), jnp.zeros(joint_bias.shape, jnp.float32), jnp.zeros((), jnp.float32))
    pieces = (grouped(encoder_out), grouped(predictor_out), grouped(labels), grouped(frame_lens), grouped(label_lens), grouped(prune_starts))
    totals, _ = lax.scan(accumulate, initial, pieces)
    return (totals[0], totals[1], totals[2], totals[3], totals[4] / BATCH)
```

```python
import functools

import jax
import jax.numpy as jnp
from jax import lax
from jax.experimental import pallas as pl
from jax.experimental.pallas import tpu as pltpu
from jax.sharding import PartitionSpec as P

S = 5
NEG_FILL = -10000.0
LOW = -1e30
F32 = jnp.float32
BF16 = jnp.bfloat16
AXES = ("zl", "x", "y", "zh", "c")
PAIRS = tuple((j, s) for s in range(S) for j in range(s + 1))


def over_rows(a, b):
    return lax.dot_general(a, b, (((0,), (0,)), ((), ())), preferred_element_type=F32)


def per_utterance(index, values):
    out = jnp.where(index == 0, values[0], values[-1])
    for b in range(1, len(values) - 1):
        out = jnp.where(index == b, values[b], out)
    return out


def shifted(rows, amount, lowest, fill):
    width = len(rows)
    span = {i: rows[i] if 0 <= i < width else fill for i in range(lowest, width + lowest + 7)}
    bits = amount - lowest
    for bit in (4, 2, 1):
        on = (bits & bit) != 0
        top = max(span)
        span = {
            i: jnp.where(on, span[i + bit], span[i])
            for i in span
            if i + bit <= top
        }
    return [span[s + lowest] for s in range(width)]


def joint_kernel(
    frames_ref, lens_ref, enc_ref, pred_ref, w_enc_ref, w_pred_ref, w_joint_ref,
    bias_ref, labels_ref, starts_ref,
    keep_ref, send_ref,
    pred_s, w_joint_s, bias_s, active_s, hidden_s, scores_s, low_s, picks_s,
    blank_s, emit_s, shift_s, terms_s, sums_s, state_s, gblank_s, grad_enc_s, grad_pred_s,
):
    count, row_count, _ = pred_ref.shape
    vocab = w_joint_ref.shape[1]
    slots = labels_ref.shape[1]
    rows = enc_ref.shape[0]
    frames = rows // count
    width = w_joint_s.shape[1]
    stride = pred_s.shape[0] // count

    frame_len = [frames_ref[b] for b in range(count)]
    label_len = [lens_ref[b] for b in range(count)]

    pred_s[...] = jnp.zeros_like(pred_s)
    for b in range(count):
        pred_s[b * stride : b * stride + row_count, :] = pred_ref[b]
    last = (width // 128 - 1) * 128
    w_joint_s[:, last:] = jnp.zeros((w_joint_s.shape[0], 128), BF16)
    w_joint_s[:, :vocab] = w_joint_ref[...]
    bias_s[...] = jnp.full_like(bias_s, LOW)
    bias_s[:, :vocab] = bias_ref[...]

    eye = lax.broadcasted_iota(jnp.int32, (frames, frames), 0) == lax.broadcasted_iota(
        jnp.int32, (frames, frames), 1
    )
    starts_f = starts_ref[...].astype(F32)
    lane_b = lax.broadcasted_iota(jnp.int32, (frames, 128), 1)
    start_cols = []
    start_tb = jnp.zeros((frames, 128), F32)
    for b in range(count):
        line = jnp.broadcast_to(starts_f[b : b + 1, :], (frames, frames))
        col = jnp.sum(jnp.where(eye, line, 0.0), axis=1, keepdims=True)
        start_cols.append(col)
        start_tb = jnp.where(lane_b == b, col, start_tb)
    start_col = jnp.concatenate(start_cols, axis=0).astype(jnp.int32)
    start_tb = start_tb.astype(jnp.int32)
    row_b = lax.broadcasted_iota(jnp.int32, (rows, 1), 0) // frames
    label_len_col = per_utterance(row_b, label_len)
    label_len_row = per_utterance(lax.broadcasted_iota(jnp.int32, (1, 128), 1), label_len)
    frame_len_row = per_utterance(lax.broadcasted_iota(jnp.int32, (1, 128), 1), frame_len)
    shift_s[0:1, :] = jnp.zeros((1, 128), jnp.int32)
    shift_s[1:frames, :] = start_tb[1:, :] - start_tb[:-1, :]

    enc_proj = jnp.dot(enc_ref[...], w_enc_ref[...], preferred_element_type=F32).astype(BF16)
    enc_proj = enc_proj.astype(F32)
    pred_proj = jnp.dot(pred_s[...], w_pred_ref[...], preferred_element_type=F32).astype(BF16)

    lane_u = lax.broadcasted_iota(jnp.int32, (rows, count * stride), 1)
    lane_k = lax.broadcasted_iota(jnp.int32, (rows, slots), 1)
    label_rows = jnp.concatenate(
        [jnp.broadcast_to(labels_ref[b : b + 1, :].astype(F32), (frames, slots)) for b in range(count)],
        axis=0,
    )
    lane_v = lax.broadcasted_iota(jnp.int32, (rows, width), 1)
    next_label, scale = [], []
    for s in range(S):
        pos = start_col + s
        pick = (lane_u == row_b * stride + pos).astype(F32).astype(BF16)
        picks_s[s] = pick
        picked = jnp.dot(pick, pred_proj, preferred_element_type=F32)
        active = jnp.tanh(enc_proj + picked)
        active_s[s] = active
        hidden = active.astype(BF16)
        hidden_s[s * rows : (s + 1) * rows, :] = hidden
        logits = jnp.dot(hidden, w_joint_s[...], preferred_element_type=F32) + bias_s[...]
        peak = jnp.max(logits, axis=1, keepdims=True)
        raised = jnp.exp(logits - peak)
        scores_s[s] = raised
        total = jnp.sum(raised, axis=1, keepdims=True)
        norm = peak + jnp.log(total)
        scale.append(1.0 / total)
        blank = jnp.where(pos <= label_len_col, logits[:, 0:1] - norm, NEG_FILL)
        blank_tb = jnp.zeros((frames, 128), F32)
        for b in range(count):
            blank_tb = jnp.where(lane_b == b, blank[b * frames : (b + 1) * frames, :], blank_tb)
        blank_s[s] = blank_tb
        if s < S - 1:
            label = jnp.sum(
                jnp.where(lane_k == pos, label_rows, 0.0), axis=1, keepdims=True
            ).astype(jnp.int32)
            next_label.append(label)
            emit = jnp.sum(jnp.where(lane_v == label, logits, 0.0), axis=1, keepdims=True)
            emit = jnp.where(pos < label_len_col, emit - norm, NEG_FILL)
            emit_tb = jnp.zeros((frames, 128), F32)
            for b in range(count):
                emit_tb = jnp.where(lane_b == b, emit[b * frames : (b + 1) * frames, :], emit_tb)
            emit_s[s] = emit_tb

    fill = jnp.full((1, 128), NEG_FILL, F32)
    state = None
    for t in range(frames):
        if t == 0:
            entering = [jnp.zeros((1, 128), F32)] + [fill] * (S - 1)
        else:
            leaving = [state[s] + blank_s[s, t - 1 : t, :] for s in range(S)]
            entering = shifted(leaving, shift_s[t : t + 1, :], -3, fill)
        emits = [emit_s[s, t : t + 1, :] for s in range(S - 1)]
        updated = []
        for s in range(S):
            routes = []
            for j in range(s + 1):
                way = entering[j]
                for i in range(j, s):
                    way = way + emits[i]
                routes.append(way)
            best = routes[0]
            for r in routes[1:]:
                best = jnp.maximum(best, r)
            terms = [jnp.exp(r - best) for r in routes]
            total = terms[0]
            for r in terms[1:]:
                total = total + r
            for j in range(s + 1):
                terms_s[PAIRS.index((j, s)), t : t + 1, :] = terms[j]
            sums_s[s, t : t + 1, :] = total
            updated.append(best + jnp.log(total))
        if t == 0:
            state = updated
        else:
            live = t < frame_len_row
            state = [jnp.where(live, n, o) for n, o in zip(updated, state)]

    frame_tb = lax.broadcasted_iota(jnp.int32, (frames, 128), 0)
    ending = frame_tb == frame_len_row - 1
    valid = lax.broadcasted_iota(jnp.int32, (1, 128), 1) < count
    final_start = jnp.sum(jnp.where(ending, start_tb.astype(F32), 0.0), axis=0, keepdims=True)
    final_pos = label_len_row - final_start.astype(jnp.int32)
    share = jnp.where(valid, -1.0 / frame_len_row.astype(F32), 0.0)
    likelihood = jnp.zeros((1, 128), F32)
    grads = []
    for s in range(S):
        here = final_pos == s
        end_blank = jnp.sum(jnp.where(ending, blank_s[s], 0.0), axis=0, keepdims=True)
        likelihood = jnp.where(here, state[s] + end_blank, likelihood)
        grads.append(jnp.where(here, share, 0.0))
        gblank_s[s] = jnp.where(ending & here, share, 0.0)
    loss = jnp.sum(jnp.where(valid, likelihood * share, 0.0), axis=1, keepdims=True)

    for s in range(S):
        inverse = 1.0 / sums_s[s]
        for j in range(s + 1):
            terms_s[PAIRS.index((j, s))] = terms_s[PAIRS.index((j, s))] * inverse

    none = jnp.zeros((1, 128), F32)
    for t in range(frames - 1, 0, -1):
        live = t < frame_len_row
        for s in range(S):
            state_s[s, t : t + 1, :] = jnp.where(live, grads[s], 0.0)
        back = []
        for j in range(S):
            parts = [grads[s] * terms_s[PAIRS.index((j, s)), t : t + 1, :] for s in range(j, S)]
            total = parts[0]
            for r in parts[1:]:
                total = total + r
            back.append(total)
        earlier = shifted(back, -shift_s[t : t + 1, :], -3, none)
        for s in range(S):
            gblank_s[s, t - 1 : t, :] += jnp.where(live, earlier[s], 0.0)
        grads = [jnp.where(live, n, o) for n, o in zip(earlier, grads)]
    for s in range(S):
        state_s[s, 0:1, :] = grads[s]

    def column(table):
        return jnp.concatenate([table[:, b : b + 1] for b in range(count)], axis=0)

    gemit = [jnp.zeros((frames, 128), F32) for _ in range(S - 1)]
    for j, s in PAIRS:
        if j < s:
            flow = state_s[s] * terms_s[PAIRS.index((j, s))]
            for i in range(j, s):
                gemit[i] = gemit[i] + flow
    bias_total = jnp.zeros((1, width), F32)
    for s in range(S):
        pos = start_col + s
        gblank = jnp.where(pos <= label_len_col, column(gblank_s[s]), 0.0)
        if s < S - 1:
            gemit_col = jnp.where(pos < label_len_col, column(gemit[s]), 0.0)
            weight = (gblank + gemit_col) * scale[s]
        else:
            weight = gblank * scale[s]
        grad = jnp.where(lane_v == 0, gblank, 0.0) - scores_s[s] * weight
        if s < S - 1:
            grad = grad + jnp.where(lane_v == next_label[s], gemit_col, 0.0)
        bias_total = bias_total + jnp.sum(grad, axis=0, keepdims=True)
        low_s[s * rows : (s + 1) * rows, :] = grad.astype(BF16)

    bias_col = jnp.transpose(jnp.broadcast_to(bias_total, (8, width)))[:, 0:1]
    row_j = lax.broadcasted_iota(jnp.int32, bias_col.shape, 0)
    side = jnp.where(row_j == width - 1, loss, bias_col)

    grad_enc_proj = jnp.zeros((rows, w_enc_ref.shape[1]), F32)
    grad_pred_proj = jnp.zeros((count * stride, w_pred_ref.shape[1]), F32)
    for s in range(S):
        grad_hidden = lax.dot_general(
            low_s[s * rows : (s + 1) * rows, :], w_joint_s[...], (((1,), (1,)), ((), ())),
            preferred_element_type=F32,
        )
        active = active_s[s]
        grad_pre = grad_hidden * (1.0 - active * active)
        grad_enc_proj = grad_enc_proj + grad_pre
        grad_pred_proj = grad_pred_proj + over_rows(picks_s[s], grad_pre.astype(BF16))
    grad_enc_s[...] = grad_enc_proj.astype(BF16)
    grad_pred_s[...] = grad_pred_proj.astype(BF16)

    core = lax.axis_index("c")
    half = width // 2
    for out_ref, which in ((send_ref, 1 - core), (keep_ref, core)):
        columns = pl.ds(pl.multiple_of(which * half, half), half)
        products = (
            over_rows(enc_ref[...], grad_enc_s[:, columns]),
            over_rows(pred_s[...], grad_pred_s[:, columns]),
            over_rows(hidden_s[...], low_s[:, columns]),
        )
        at = 0
        for m, product in enumerate(products):
            if m == 2:
                lane = lax.broadcasted_iota(jnp.int32, product.shape, 1) + which * half
                product = jnp.where(lane == vocab, side, product)
            for j in range(half // 128):
                out_ref[at : at + width, :] = product[:, j * 128 : (j + 1) * 128]
                at += width


def local_grads(
    encoder_out, predictor_out, w_encoder, w_predictor, w_joint, joint_bias,
    labels, frame_lens, label_lens, prune_starts,
):
    count, frames, enc_width = encoder_out.shape
    pred_width = predictor_out.shape[2]
    joint_width, vocab = w_joint.shape
    rows = count * frames
    width = -(-vocab // 128) * 128
    stride = 32
    vmem = pl.BlockSpec(memory_space=pltpu.VMEM)
    smem = pl.BlockSpec(memory_space=pltpu.SMEM)
    return pl.pallas_call(
        joint_kernel,
        out_shape=(jax.ShapeDtypeStruct((3 * width * width // 256, 128), F32),) * 2,
        in_specs=[smem, smem] + [vmem] * 8,
        out_specs=(vmem, vmem),
        scratch_shapes=[
            pltpu.VMEM((count * stride, pred_width), BF16),
            pltpu.VMEM((joint_width, width), BF16),
            pltpu.VMEM((1, width), F32),
            pltpu.VMEM((S, rows, joint_width), F32),
            pltpu.VMEM((S * rows, joint_width), BF16),
            pltpu.VMEM((S, rows, width), F32),
            pltpu.VMEM((S * rows, width), BF16),
            pltpu.VMEM((S, rows, count * stride), BF16),
            pltpu.VMEM((S, frames, 128), F32),
            pltpu.VMEM((S - 1, frames, 128), F32),
            pltpu.VMEM((frames, 128), jnp.int32),
            pltpu.VMEM((len(PAIRS), frames, 128), F32),
            pltpu.VMEM((S, frames, 128), F32),
            pltpu.VMEM((S, frames, 128), F32),
            pltpu.VMEM((S, frames, 128), F32),
            pltpu.VMEM((rows, joint_width), BF16),
            pltpu.VMEM((count * stride, joint_width), BF16),
        ],
        name="joint",
    )(
        frame_lens, label_lens, encoder_out.reshape(rows, enc_width), predictor_out,
        w_encoder, w_predictor, w_joint, joint_bias.reshape(1, vocab), labels, prune_starts,
    )


def unpack_kernel(utterances, mine_ref, other_ref, enc_ref, pred_ref, joint_ref, bias_ref, loss_ref):
    core = lax.axis_index("c")
    width = enc_ref.shape[0]
    vocab = joint_ref.shape[1]
    half = width // 256

    def place(refs):
        for h in range(2):
            for m, out_ref in enumerate((enc_ref, pred_ref, joint_ref)):
                for j in range(half):
                    at = (m * half + j) * width
                    lane = (h * half + j) * 128
                    size = min(128, out_ref.shape[1] - lane)
                    out_ref[:, lane : lane + size] = refs[h][at : at + width, :size]
        at = (2 * half + (vocab // 128) % half) * width
        tile = refs[vocab // 128 // half][at : at + width, :]
        side = jnp.transpose(tile)[vocab % 128 : vocab % 128 + 1, :]
        bias_ref[...] = side[:, :vocab]
        loss_ref[...] = side[:, width - 1 :] / utterances

    @pl.when(core == 0)
    def _():
        place((mine_ref, other_ref))

    @pl.when(core != 0)
    def _():
        place((other_ref, mine_ref))


def swap_cores(value):
    return lax.ppermute(value, "c", [(0, 1), (1, 0)])


def sum_at_owner(value, axes):
    members = lax.axis_size(axes)
    arrived = lax.all_to_all(value, axes, split_axis=0, concat_axis=0, tiled=True)
    return arrived.reshape(members, -1, value.shape[1]).sum(axis=0)


def from_all(value, axes):
    members = lax.axis_size(axes)
    spread = jnp.broadcast_to(value[None], (members, *value.shape))
    spread = spread.reshape(-1, value.shape[1])
    return lax.all_to_all(spread, axes, split_axis=0, concat_axis=0, tiled=True)


def shards(*args):
    keep, send = local_grads(*args)
    mine = keep + swap_cores(send)
    mine = sum_at_owner(mine, ("x", "y"))
    mine = sum_at_owner(mine, ("zl", "zh"))
    mine = from_all(mine, ("zl", "zh"))
    mine = from_all(mine, ("x", "y"))
    other = swap_cores(mine)
    width, vocab = args[4].shape
    utterances = args[0].shape[0] * lax.axis_size(AXES)
    vmem = pl.BlockSpec(memory_space=pltpu.VMEM)
    grad_encoder, grad_predictor, grad_joint, grad_bias, loss = pl.pallas_call(
        functools.partial(unpack_kernel, utterances),
        out_shape=(
            jax.ShapeDtypeStruct((width, width), F32),
            jax.ShapeDtypeStruct((width, width), F32),
            jax.ShapeDtypeStruct((width, vocab), F32),
            jax.ShapeDtypeStruct((1, vocab), F32),
            jax.ShapeDtypeStruct((1, 1), F32),
        ),
        in_specs=[vmem, vmem],
        out_specs=(vmem,) * 5,
        name="unpack",
    )(mine, other)
    return grad_encoder, grad_predictor, grad_joint, grad_bias.reshape(vocab), loss.reshape(())


def solution(mesh):
    mesh = jax.sharding.Mesh(mesh.devices.reshape(4, 4, 4, 2, 2), AXES)
    in_specs = (
        P(AXES, None, None), P(AXES, None, None), P(), P(), P(), P(),
        P(AXES, None), P(AXES), P(AXES), P(AXES, None),
    )
    return jax.shard_map(
        shards, mesh=mesh, in_specs=in_specs, out_specs=(P(),) * 5, check_vma=False
    )
```

```python
import functools

import jax
import jax.numpy as jnp
from jax import lax
from jax.experimental import pallas as pl
from jax.experimental.pallas import tpu as pltpu
from jax.sharding import PartitionSpec as P

S = 5
NEG_FILL = -10000.0
LOW = -1e30
F32 = jnp.float32
BF16 = jnp.bfloat16
AXES = ("zq", "zp", "x", "y", "zh", "c")
NEAR = ("zp", "x", "y")
FAR = ("zq", "zh")
PAIRS = tuple((j, s) for s in range(S) for j in range(s + 1))


def over_rows(a, b):
    return lax.dot_general(a, b, (((0,), (0,)), ((), ())), preferred_element_type=F32)


def per_utterance(index, values):
    out = jnp.where(index == 0, values[0], values[-1])
    for b in range(1, len(values) - 1):
        out = jnp.where(index == b, values[b], out)
    return out


def shifted(rows, amount, lowest, fill):
    width = len(rows)
    span = {i: rows[i] if 0 <= i < width else fill for i in range(lowest, width + lowest + 7)}
    bits = amount - lowest
    for bit in (4, 2, 1):
        on = (bits & bit) != 0
        top = max(span)
        span = {
            i: jnp.where(on, span[i + bit], span[i])
            for i in span
            if i + bit <= top
        }
    return [span[s + lowest] for s in range(width)]


def joint_kernel(
    frames_hbm, lens_hbm, enc_hbm, pred_hbm, w_enc_hbm, w_pred_hbm, w_joint_hbm,
    bias_hbm, labels_hbm, starts_hbm,
    keep_ref, send_ref,
    frames_ref, lens_ref, enc_ref, pred_ref, w_enc_ref, w_pred_ref, w_joint_ref,
    bias_ref, labels_ref, starts_ref, load_sems,
    pred_s, w_joint_s, bias_s, active_s, hidden_s, scores_s, low_s, picks_s,
    blank_s, emit_s, shift_s, terms_s, sums_s, state_s, gblank_s, grad_enc_s, grad_pred_s,
):
    loads = {
        name: pltpu.make_async_copy(src, dst, load_sems.at[i])
        for i, (name, src, dst) in enumerate((
            ("starts", starts_hbm, starts_ref),
            ("frames", frames_hbm, frames_ref),
            ("lens", lens_hbm, lens_ref),
            ("enc", enc_hbm, enc_ref),
            ("w_enc", w_enc_hbm, w_enc_ref),
            ("pred", pred_hbm, pred_ref),
            ("w_pred", w_pred_hbm, w_pred_ref),
            ("labels", labels_hbm, labels_ref),
            ("bias", bias_hbm, bias_ref),
            ("w_joint", w_joint_hbm, w_joint_ref),
        ))
    }
    for load in loads.values():
        load.start()

    row_count, count, _ = pred_ref.shape
    vocab = w_joint_ref.shape[0]
    slots = labels_ref.shape[1]
    rows = enc_ref.shape[0]
    frames = rows // count
    width = w_joint_s.shape[0]
    places = pred_s.shape[0]

    pred_s[...] = jnp.zeros_like(pred_s)
    last = (width // 128 - 1) * 128
    w_joint_s[last:, :] = jnp.zeros((128, w_joint_s.shape[1]), BF16)
    bias_s[...] = jnp.full_like(bias_s, LOW)
    for name in ("starts", "frames", "lens"):
        loads[name].wait()
    frame_len = [frames_ref[b] for b in range(count)]
    label_len = [lens_ref[b] for b in range(count)]

    eye = lax.broadcasted_iota(jnp.int32, (frames, frames), 0) == lax.broadcasted_iota(
        jnp.int32, (frames, frames), 1
    )
    starts_f = starts_ref[...].astype(F32)
    lane_b = lax.broadcasted_iota(jnp.int32, (frames, 128), 1)
    start_cols = []
    start_tb = jnp.zeros((frames, 128), F32)
    for b in range(count):
        line = jnp.broadcast_to(starts_f[b : b + 1, :], (frames, frames))
        col = jnp.sum(jnp.where(eye, line, 0.0), axis=1, keepdims=True)
        start_cols.append(col)
        start_tb = jnp.where(lane_b == b, col, start_tb)
    start_col = jnp.concatenate(start_cols, axis=0).astype(jnp.int32)
    start_tb = start_tb.astype(jnp.int32)
    row_b = lax.broadcasted_iota(jnp.int32, (rows, 1), 0) // frames
    label_len_col = per_utterance(row_b, label_len)
    label_len_row = per_utterance(lax.broadcasted_iota(jnp.int32, (1, 128), 1), label_len)
    frame_len_row = per_utterance(lax.broadcasted_iota(jnp.int32, (1, 128), 1), frame_len)
    shift_s[0:1, :] = jnp.zeros((1, 128), jnp.int32)
    shift_s[1:frames, :] = start_tb[1:, :] - start_tb[:-1, :]

    for name in ("enc", "w_enc", "pred", "w_pred"):
        loads[name].wait()
    for u in range(row_count):
        pred_s[u * count : (u + 1) * count, :] = pred_ref[u]
    enc_proj = jnp.dot(enc_ref[...], w_enc_ref[...], preferred_element_type=F32).astype(BF16)
    enc_proj = enc_proj.astype(F32)
    pred_proj = jnp.dot(pred_s[...], w_pred_ref[...], preferred_element_type=F32).astype(BF16)

    for name in ("labels", "bias", "w_joint"):
        loads[name].wait()
    w_joint_s[:vocab, :] = w_joint_ref[...]
    bias_s[:, :vocab] = bias_ref[...]
    lane_u = lax.broadcasted_iota(jnp.int32, (rows, places), 1)
    lane_k = lax.broadcasted_iota(jnp.int32, (rows, slots), 1)
    label_rows = jnp.concatenate(
        [jnp.broadcast_to(labels_ref[b : b + 1, :].astype(F32), (frames, slots)) for b in range(count)],
        axis=0,
    )
    lane_v = lax.broadcasted_iota(jnp.int32, (rows, width), 1)
    next_label, scale = [], []
    for s in range(S):
        pos = start_col + s
        pick = (lane_u == pos * count + row_b).astype(F32).astype(BF16)
        picks_s[s] = pick
        picked = jnp.dot(pick, pred_proj, preferred_element_type=F32)
        active = jnp.tanh(enc_proj + picked)
        active_s[s] = active
        hidden = active.astype(BF16)
        hidden_s[s * rows : (s + 1) * rows, :] = hidden
        logits = lax.dot_general(
            hidden, w_joint_s[...], (((1,), (1,)), ((), ())), preferred_element_type=F32
        )
        logits = logits + bias_s[...]
        peak = jnp.max(logits, axis=1, keepdims=True)
        raised = jnp.exp(logits - peak)
        scores_s[s] = raised
        total = jnp.sum(raised, axis=1, keepdims=True)
        norm = peak + jnp.log(total)
        scale.append(1.0 / total)
        blank = jnp.where(pos <= label_len_col, logits[:, 0:1] - norm, NEG_FILL)
        blank_tb = jnp.zeros((frames, 128), F32)
        for b in range(count):
            blank_tb = jnp.where(lane_b == b, blank[b * frames : (b + 1) * frames, :], blank_tb)
        blank_s[s] = blank_tb
        if s < S - 1:
            label = jnp.sum(
                jnp.where(lane_k == pos, label_rows, 0.0), axis=1, keepdims=True
            ).astype(jnp.int32)
            next_label.append(label)
            emit = jnp.sum(jnp.where(lane_v == label, logits, 0.0), axis=1, keepdims=True)
            emit = jnp.where(pos < label_len_col, emit - norm, NEG_FILL)
            emit_tb = jnp.zeros((frames, 128), F32)
            for b in range(count):
                emit_tb = jnp.where(lane_b == b, emit[b * frames : (b + 1) * frames, :], emit_tb)
            emit_s[s] = emit_tb

    fill = jnp.full((1, 128), NEG_FILL, F32)
    state = None
    for t in range(frames):
        if t == 0:
            entering = [jnp.zeros((1, 128), F32)] + [fill] * (S - 1)
        else:
            leaving = [state[s] + blank_s[s, t - 1 : t, :] for s in range(S)]
            entering = shifted(leaving, shift_s[t : t + 1, :], -3, fill)
        emits = [emit_s[s, t : t + 1, :] for s in range(S - 1)]
        updated = []
        for s in range(S):
            routes = []
            for j in range(s + 1):
                way = entering[j]
                for i in range(j, s):
                    way = way + emits[i]
                routes.append(way)
            best = routes[0]
            for r in routes[1:]:
                best = jnp.maximum(best, r)
            terms = [jnp.exp(r - best) for r in routes]
            total = terms[0]
            for r in terms[1:]:
                total = total + r
            for j in range(s + 1):
                terms_s[PAIRS.index((j, s)), t : t + 1, :] = terms[j]
            sums_s[s, t : t + 1, :] = total
            updated.append(best + jnp.log(total))
        if t == 0:
            state = updated
        else:
            live = t < frame_len_row
            state = [jnp.where(live, n, o) for n, o in zip(updated, state)]

    frame_tb = lax.broadcasted_iota(jnp.int32, (frames, 128), 0)
    ending = frame_tb == frame_len_row - 1
    valid = lax.broadcasted_iota(jnp.int32, (1, 128), 1) < count
    final_start = jnp.sum(jnp.where(ending, start_tb.astype(F32), 0.0), axis=0, keepdims=True)
    final_pos = label_len_row - final_start.astype(jnp.int32)
    share = jnp.where(valid, -1.0 / frame_len_row.astype(F32), 0.0)
    likelihood = jnp.zeros((1, 128), F32)
    grads = []
    for s in range(S):
        here = final_pos == s
        end_blank = jnp.sum(jnp.where(ending, blank_s[s], 0.0), axis=0, keepdims=True)
        likelihood = jnp.where(here, state[s] + end_blank, likelihood)
        grads.append(jnp.where(here, share, 0.0))
        gblank_s[s] = jnp.where(ending & here, share, 0.0)
    loss = jnp.sum(jnp.where(valid, likelihood * share, 0.0), axis=1, keepdims=True)

    for s in range(S):
        inverse = 1.0 / sums_s[s]
        for j in range(s + 1):
            terms_s[PAIRS.index((j, s))] = terms_s[PAIRS.index((j, s))] * inverse

    none = jnp.zeros((1, 128), F32)
    for t in range(frames - 1, 0, -1):
        live = t < frame_len_row
        for s in range(S):
            state_s[s, t : t + 1, :] = jnp.where(live, grads[s], 0.0)
        back = []
        for j in range(S):
            parts = [grads[s] * terms_s[PAIRS.index((j, s)), t : t + 1, :] for s in range(j, S)]
            total = parts[0]
            for r in parts[1:]:
                total = total + r
            back.append(total)
        earlier = shifted(back, -shift_s[t : t + 1, :], -3, none)
        for s in range(S):
            gblank_s[s, t - 1 : t, :] += jnp.where(live, earlier[s], 0.0)
        grads = [jnp.where(live, n, o) for n, o in zip(earlier, grads)]
    for s in range(S):
        state_s[s, 0:1, :] = grads[s]

    def column(table):
        return jnp.concatenate([table[:, b : b + 1] for b in range(count)], axis=0)

    gemit = [jnp.zeros((frames, 128), F32) for _ in range(S - 1)]
    for j, s in PAIRS:
        if j < s:
            flow = state_s[s] * terms_s[PAIRS.index((j, s))]
            for i in range(j, s):
                gemit[i] = gemit[i] + flow
    bias_total = jnp.zeros((1, width), F32)
    for s in range(S):
        pos = start_col + s
        gblank = jnp.where(pos <= label_len_col, column(gblank_s[s]), 0.0)
        if s < S - 1:
            gemit_col = jnp.where(pos < label_len_col, column(gemit[s]), 0.0)
            weight = (gblank + gemit_col) * scale[s]
        else:
            weight = gblank * scale[s]
        grad = jnp.where(lane_v == 0, gblank, 0.0) - scores_s[s] * weight
        if s < S - 1:
            grad = grad + jnp.where(lane_v == next_label[s], gemit_col, 0.0)
        bias_total = bias_total + jnp.sum(grad, axis=0, keepdims=True)
        low_s[s * rows : (s + 1) * rows, :] = grad.astype(BF16)

    grad_enc_proj = jnp.zeros((rows, w_enc_ref.shape[1]), F32)
    grad_pred_proj = jnp.zeros((places, w_pred_ref.shape[1]), F32)
    for s in range(S):
        grad_hidden = jnp.dot(
            low_s[s * rows : (s + 1) * rows, :], w_joint_s[...], preferred_element_type=F32
        )
        active = active_s[s]
        grad_pre = grad_hidden * (1.0 - active * active)
        grad_enc_proj = grad_enc_proj + grad_pre
        grad_pred_proj = grad_pred_proj + over_rows(picks_s[s], grad_pre.astype(BF16))
    bias_s[...] = bias_total
    grad_enc_s[...] = grad_enc_proj.astype(BF16)
    grad_pred_s[...] = grad_pred_proj.astype(BF16)

    core = lax.axis_index("c")
    half = width // 2
    for out_ref, which in ((send_ref, 1 - core), (keep_ref, core)):
        columns = pl.ds(pl.multiple_of(which * half, half), half)
        products = (
            over_rows(enc_ref[...], grad_enc_s[:, columns]),
            over_rows(pred_s[...], grad_pred_s[:, columns]),
            over_rows(low_s[...], hidden_s[:, columns]),
        )
        at = 0
        for product in products:
            for j in range(half // 128):
                out_ref[at : at + width, :] = product[:, j * 128 : (j + 1) * 128]
                at += width
        base = at - (half // 128) * width + vocab
        for j in range(half // 128):
            lanes = pl.ds(pl.multiple_of(which * half + j * 128, 128), 128)
            out_ref[base + j * width : base + j * width + 1, :] = bias_s[:, lanes]
            out_ref[base + j * width + 1 : base + j * width + 2, :] = jnp.broadcast_to(loss, (1, 128))


def local_grads(
    encoder_out, predictor_out, w_encoder, w_predictor, w_joint, joint_bias,
    labels, frame_lens, label_lens, prune_starts,
):
    count, frames, enc_width = encoder_out.shape
    pred_width = predictor_out.shape[2]
    joint_width, vocab = w_joint.shape
    rows = count * frames
    width = -(-vocab // 128) * 128
    places = 128
    vmem = pl.BlockSpec(memory_space=pltpu.VMEM)
    return pl.pallas_call(
        joint_kernel,
        out_shape=(pltpu.VMEM((3 * width * width // 256, 128), F32),) * 2,
        in_specs=[pl.BlockSpec(memory_space=pltpu.HBM)] * 10,
        out_specs=(vmem, vmem),
        scratch_shapes=[
            pltpu.SMEM((count,), jnp.int32),
            pltpu.SMEM((count,), jnp.int32),
            pltpu.VMEM((rows, enc_width), BF16),
            pltpu.VMEM((predictor_out.shape[1], count, pred_width), BF16),
            pltpu.VMEM(w_encoder.shape, BF16),
            pltpu.VMEM(w_predictor.shape, BF16),
            pltpu.VMEM((vocab, joint_width), BF16),
            pltpu.VMEM((1, vocab), F32),
            pltpu.VMEM(labels.shape, jnp.int32),
            pltpu.VMEM(prune_starts.shape, jnp.int32),
            pltpu.SemaphoreType.DMA((10,)),
            pltpu.VMEM((places, pred_width), BF16),
            pltpu.VMEM((width, joint_width), BF16),
            pltpu.VMEM((1, width), F32),
            pltpu.VMEM((S, rows, joint_width), F32),
            pltpu.VMEM((S * rows, joint_width), BF16),
            pltpu.VMEM((S, rows, width), F32),
            pltpu.VMEM((S * rows, width), BF16),
            pltpu.VMEM((S, rows, places), BF16),
            pltpu.VMEM((S, frames, 128), F32),
            pltpu.VMEM((S - 1, frames, 128), F32),
            pltpu.VMEM((frames, 128), jnp.int32),
            pltpu.VMEM((len(PAIRS), frames, 128), F32),
            pltpu.VMEM((S, frames, 128), F32),
            pltpu.VMEM((S, frames, 128), F32),
            pltpu.VMEM((S, frames, 128), F32),
            pltpu.VMEM((rows, joint_width), BF16),
            pltpu.VMEM((places, joint_width), BF16),
        ],
        compiler_params=pltpu.CompilerParams(vmem_limit_bytes=56 * 2**20),
        name="joint",
    )(
        frame_lens, label_lens, encoder_out.reshape(rows, enc_width),
        jnp.swapaxes(predictor_out, 0, 1),        w_encoder, w_predictor, w_joint.T, joint_bias.reshape(1, vocab), labels, prune_starts,
    )


def unpack_kernel(utterances, mine_ref, other_ref, enc_ref, pred_ref, joint_ref, bias_ref, loss_ref):
    core = lax.axis_index("c")
    width = enc_ref.shape[0]
    vocab = joint_ref.shape[0]
    half = width // 256

    def place(refs):
        for h in range(2):
            for m, out_ref in enumerate((enc_ref, pred_ref, joint_ref)):
                for j in range(half):
                    at = (m * half + j) * width
                    lane = (h * half + j) * 128
                    size = out_ref.shape[0]
                    out_ref[:, lane : lane + 128] = refs[h][at : at + size, :]
            for j in range(half):
                at = (2 * half + j) * width + vocab
                lane = (h * half + j) * 128
                size = min(128, vocab - lane)
                bias_ref[:, lane : lane + size] = refs[h][at : at + 1, :size]
        at = 2 * half * width + vocab + 1
        loss_ref[...] = refs[0][at : at + 1, 0:1] / utterances

    @pl.when(core == 0)
    def _():
        place((mine_ref, other_ref))

    @pl.when(core != 0)
    def _():
        place((other_ref, mine_ref))


def swap_cores(value):
    return lax.ppermute(value, "c", [(0, 1), (1, 0)])


def sum_at_owner(value, axes):
    members = lax.axis_size(axes)
    arrived = lax.all_to_all(value, axes, split_axis=0, concat_axis=0, tiled=True)
    return arrived.reshape(members, -1, value.shape[1]).sum(axis=0)


def from_all(value, axes):
    members = lax.axis_size(axes)
    spread = jnp.broadcast_to(value[None], (members, *value.shape))
    spread = spread.reshape(-1, value.shape[1])
    return lax.all_to_all(spread, axes, split_axis=0, concat_axis=0, tiled=True)


def sum_everywhere(value, axes):
    sizes = [lax.axis_size(a) for a in axes]
    assert sizes == [2, 2]
    arrived = []
    for step in (2, 1, 3):
        pairs = [
            (2 * (n % 2) + n // 2, 2 * ((n + step) % 4 % 2) + (n + step) % 4 // 2)
            for n in range(4)
        ]
        arrived.append(lax.ppermute(value, axes, pairs))
    return (value + arrived[0]) + (arrived[1] + arrived[2])


def shards(*args):
    keep, send = local_grads(*args)
    mine = keep + swap_cores(send)
    mine = sum_at_owner(mine, NEAR)
    mine = sum_everywhere(mine, FAR)
    mine = from_all(mine, NEAR)
    other = swap_cores(mine)
    width, vocab = args[4].shape
    utterances = args[0].shape[0] * lax.axis_size(AXES)
    vmem = pl.BlockSpec(memory_space=pltpu.VMEM)
    grad_encoder, grad_predictor, grad_joint, grad_bias, loss = pl.pallas_call(
        functools.partial(unpack_kernel, utterances),
        out_shape=(
            jax.ShapeDtypeStruct((width, width), F32),
            jax.ShapeDtypeStruct((width, width), F32),
            jax.ShapeDtypeStruct((vocab, width), F32),
            jax.ShapeDtypeStruct((1, vocab), F32),
            jax.ShapeDtypeStruct((1, 1), F32),
        ),
        in_specs=[vmem, vmem],
        out_specs=(vmem,) * 5,
        compiler_params=pltpu.CompilerParams(vmem_limit_bytes=20 * 2**20),
        name="unpack",
    )(mine, other)
    return grad_encoder, grad_predictor, grad_joint.T, grad_bias.reshape(vocab), loss.reshape(())


def solution(mesh):
    mesh = jax.sharding.Mesh(mesh.devices.reshape(2, 2, 4, 4, 2, 2), AXES)
    in_specs = (
        P(AXES, None, None), P(AXES, None, None), P(), P(), P(), P(),
        P(AXES, None), P(AXES), P(AXES), P(AXES, None),
    )
    return jax.shard_map(
        shards, mesh=mesh, in_specs=in_specs, out_specs=(P(),) * 5, check_vma=False
    )
```

```python
import functools

import jax
import jax.numpy as jnp
from jax import lax
from jax.experimental import pallas as pl
from jax.experimental.pallas import tpu as pltpu
from jax.sharding import PartitionSpec as P

S = 5
NEG_FILL = -10000.0
LOW = -1e30
F32 = jnp.float32
BF16 = jnp.bfloat16
AXES = ("zq", "zp", "x", "y", "zh", "c")
NEAR = ("zp", "x", "y")
FAR = ("zq", "zh")
SECOND = 0
STAGGER = 900
PAIRS = tuple((j, s) for s in range(S) for j in range(s + 1))


def over_rows(a, b):
    return lax.dot_general(a, b, (((0,), (0,)), ((), ())), preferred_element_type=F32)


def per_utterance(index, values):
    out = jnp.where(index == 0, values[0], values[-1])
    for b in range(1, len(values) - 1):
        out = jnp.where(index == b, values[b], out)
    return out


def shifted(rows, amount, lowest, fill):
    width = len(rows)
    span = {i: rows[i] if 0 <= i < width else fill for i in range(lowest, width + lowest + 7)}
    bits = amount - lowest
    for bit in (4, 2, 1):
        on = (bits & bit) != 0
        top = max(span)
        span = {
            i: jnp.where(on, span[i + bit], span[i])
            for i in span
            if i + bit <= top
        }
    return [span[s + lowest] for s in range(width)]


def joint_kernel(
    frames_hbm, lens_hbm, enc_hbm, pred_hbm, w_enc_hbm, w_pred_hbm, w_joint_hbm,
    bias_hbm, labels_hbm, starts_hbm,
    keep_ref, send_ref,
    frames_ref, lens_ref, enc_ref, pred_ref, w_enc_ref, w_pred_ref, w_joint_ref,
    bias_ref, labels_ref, starts_ref, load_sems,
    pred_s, w_joint_s, bias_s, active_s, hidden_s, scores_s, low_s, picks_s,
    blank_s, emit_s, shift_s, terms_s, sums_s, state_s, gblank_s, grad_enc_s, grad_pred_s,
):
    loads = {
        name: pltpu.make_async_copy(src, dst, load_sems.at[i])
        for i, (name, src, dst) in enumerate((
            ("starts", starts_hbm, starts_ref),
            ("frames", frames_hbm, frames_ref),
            ("lens", lens_hbm, lens_ref),
            ("enc", enc_hbm, enc_ref),
            ("w_enc", w_enc_hbm, w_enc_ref),
            ("pred", pred_hbm, pred_ref),
            ("w_pred", w_pred_hbm, w_pred_ref),
            ("labels", labels_hbm, labels_ref),
            ("bias", bias_hbm, bias_ref),
            ("w_joint", w_joint_hbm, w_joint_ref),
        ))
    }
    for load in loads.values():
        load.start()

    row_count, count, _ = pred_ref.shape
    vocab = w_joint_ref.shape[0]
    slots = labels_ref.shape[1]
    rows = enc_ref.shape[0]
    frames = rows // count
    width = w_joint_s.shape[0]
    places = pred_s.shape[0]

    pred_s[...] = jnp.zeros_like(pred_s)
    last = (width // 128 - 1) * 128
    w_joint_s[last:, :] = jnp.zeros((128, w_joint_s.shape[1]), BF16)
    bias_s[...] = jnp.full_like(bias_s, LOW)
    for name in ("starts", "frames", "lens"):
        loads[name].wait()
    frame_len = [frames_ref[b] for b in range(count)]
    label_len = [lens_ref[b] for b in range(count)]

    eye = lax.broadcasted_iota(jnp.int32, (frames, frames), 0) == lax.broadcasted_iota(
        jnp.int32, (frames, frames), 1
    )
    starts_f = starts_ref[...].astype(F32)
    lane_b = lax.broadcasted_iota(jnp.int32, (frames, 128), 1)
    start_cols = []
    start_tb = jnp.zeros((frames, 128), F32)
    for b in range(count):
        line = jnp.broadcast_to(starts_f[b : b + 1, :], (frames, frames))
        col = jnp.sum(jnp.where(eye, line, 0.0), axis=1, keepdims=True)
        start_cols.append(col)
        start_tb = jnp.where(lane_b == b, col, start_tb)
    start_col = jnp.concatenate(start_cols, axis=0).astype(jnp.int32)
    start_tb = start_tb.astype(jnp.int32)
    row_b = lax.broadcasted_iota(jnp.int32, (rows, 1), 0) // frames
    label_len_col = per_utterance(row_b, label_len)
    label_len_row = per_utterance(lax.broadcasted_iota(jnp.int32, (1, 128), 1), label_len)
    frame_len_row = per_utterance(lax.broadcasted_iota(jnp.int32, (1, 128), 1), frame_len)
    shift_s[0:1, :] = jnp.zeros((1, 128), jnp.int32)
    shift_s[1:frames, :] = start_tb[1:, :] - start_tb[:-1, :]

    for name in ("enc", "w_enc", "pred", "w_pred"):
        loads[name].wait()
    for u in range(row_count):
        pred_s[u * count : (u + 1) * count, :] = pred_ref[u]
    enc_proj = jnp.dot(enc_ref[...], w_enc_ref[...], preferred_element_type=F32).astype(BF16)
    enc_proj = enc_proj.astype(F32)
    pred_proj = jnp.dot(pred_s[...], w_pred_ref[...], preferred_element_type=F32).astype(BF16)

    for name in ("labels", "bias", "w_joint"):
        loads[name].wait()
    w_joint_s[:vocab, :] = w_joint_ref[...]
    bias_s[:, :vocab] = bias_ref[...]
    lane_u = lax.broadcasted_iota(jnp.int32, (rows, places), 1)
    lane_k = lax.broadcasted_iota(jnp.int32, (rows, slots), 1)
    label_rows = jnp.concatenate(
        [jnp.broadcast_to(labels_ref[b : b + 1, :].astype(F32), (frames, slots)) for b in range(count)],
        axis=0,
    )
    lane_v = lax.broadcasted_iota(jnp.int32, (rows, width), 1)
    next_label, scale = [], []
    for s in range(S):
        pos = start_col + s
        pick = (lane_u == pos * count + row_b).astype(F32).astype(BF16)
        picks_s[s] = pick
        picked = jnp.dot(pick, pred_proj, preferred_element_type=F32)
        active = jnp.tanh(enc_proj + picked)
        active_s[s] = active
        hidden = active.astype(BF16)
        hidden_s[s * rows : (s + 1) * rows, :] = hidden
        logits = lax.dot_general(
            hidden, w_joint_s[...], (((1,), (1,)), ((), ())), preferred_element_type=F32
        )
        logits = logits + bias_s[...]
        peak = jnp.max(logits, axis=1, keepdims=True)
        raised = jnp.exp(logits - peak)
        scores_s[s] = raised
        total = jnp.sum(raised, axis=1, keepdims=True)
        norm = peak + jnp.log(total)
        scale.append(1.0 / total)
        blank = jnp.where(pos <= label_len_col, logits[:, 0:1] - norm, NEG_FILL)
        blank_tb = jnp.zeros((frames, 128), F32)
        for b in range(count):
            blank_tb = jnp.where(lane_b == b, blank[b * frames : (b + 1) * frames, :], blank_tb)
        blank_s[s] = blank_tb
        if s < S - 1:
            label = jnp.sum(
                jnp.where(lane_k == pos, label_rows, 0.0), axis=1, keepdims=True
            ).astype(jnp.int32)
            next_label.append(label)
            emit = jnp.sum(jnp.where(lane_v == label, logits, 0.0), axis=1, keepdims=True)
            emit = jnp.where(pos < label_len_col, emit - norm, NEG_FILL)
            emit_tb = jnp.zeros((frames, 128), F32)
            for b in range(count):
                emit_tb = jnp.where(lane_b == b, emit[b * frames : (b + 1) * frames, :], emit_tb)
            emit_s[s] = emit_tb

    fill = jnp.full((1, 128), NEG_FILL, F32)
    state = None
    for t in range(frames):
        if t == 0:
            entering = [jnp.zeros((1, 128), F32)] + [fill] * (S - 1)
        else:
            leaving = [state[s] + blank_s[s, t - 1 : t, :] for s in range(S)]
            entering = shifted(leaving, shift_s[t : t + 1, :], -3, fill)
        emits = [emit_s[s, t : t + 1, :] for s in range(S - 1)]
        updated = []
        for s in range(S):
            routes = []
            for j in range(s + 1):
                way = entering[j]
                for i in range(j, s):
                    way = way + emits[i]
                routes.append(way)
            best = routes[0]
            for r in routes[1:]:
                best = jnp.maximum(best, r)
            terms = [jnp.exp(r - best) for r in routes]
            total = terms[0]
            for r in terms[1:]:
                total = total + r
            for j in range(s + 1):
                terms_s[PAIRS.index((j, s)), t : t + 1, :] = terms[j]
            sums_s[s, t : t + 1, :] = total
            updated.append(best + jnp.log(total))
        if t == 0:
            state = updated
        else:
            live = t < frame_len_row
            state = [jnp.where(live, n, o) for n, o in zip(updated, state)]

    frame_tb = lax.broadcasted_iota(jnp.int32, (frames, 128), 0)
    ending = frame_tb == frame_len_row - 1
    valid = lax.broadcasted_iota(jnp.int32, (1, 128), 1) < count
    final_start = jnp.sum(jnp.where(ending, start_tb.astype(F32), 0.0), axis=0, keepdims=True)
    final_pos = label_len_row - final_start.astype(jnp.int32)
    share = jnp.where(valid, -1.0 / frame_len_row.astype(F32), 0.0)
    likelihood = jnp.zeros((1, 128), F32)
    grads = []
    for s in range(S):
        here = final_pos == s
        end_blank = jnp.sum(jnp.where(ending, blank_s[s], 0.0), axis=0, keepdims=True)
        likelihood = jnp.where(here, state[s] + end_blank, likelihood)
        grads.append(jnp.where(here, share, 0.0))
        gblank_s[s] = jnp.where(ending & here, share, 0.0)
    loss = jnp.sum(jnp.where(valid, likelihood * share, 0.0), axis=1, keepdims=True)

    for s in range(S):
        inverse = 1.0 / sums_s[s]
        for j in range(s + 1):
            terms_s[PAIRS.index((j, s))] = terms_s[PAIRS.index((j, s))] * inverse

    none = jnp.zeros((1, 128), F32)
    for t in range(frames - 1, 0, -1):
        live = t < frame_len_row
        for s in range(S):
            state_s[s, t : t + 1, :] = jnp.where(live, grads[s], 0.0)
        back = []
        for j in range(S):
            parts = [grads[s] * terms_s[PAIRS.index((j, s)), t : t + 1, :] for s in range(j, S)]
            total = parts[0]
            for r in parts[1:]:
                total = total + r
            back.append(total)
        earlier = shifted(back, -shift_s[t : t + 1, :], -3, none)
        for s in range(S):
            gblank_s[s, t - 1 : t, :] += jnp.where(live, earlier[s], 0.0)
        grads = [jnp.where(live, n, o) for n, o in zip(earlier, grads)]
    for s in range(S):
        state_s[s, 0:1, :] = grads[s]

    def column(table):
        return jnp.concatenate([table[:, b : b + 1] for b in range(count)], axis=0)

    gemit = [jnp.zeros((frames, 128), F32) for _ in range(S - 1)]
    for j, s in PAIRS:
        if j < s:
            flow = state_s[s] * terms_s[PAIRS.index((j, s))]
            for i in range(j, s):
                gemit[i] = gemit[i] + flow
    bias_total = jnp.zeros((1, width), F32)
    for s in range(S):
        pos = start_col + s
        gblank = jnp.where(pos <= label_len_col, column(gblank_s[s]), 0.0)
        if s < S - 1:
            gemit_col = jnp.where(pos < label_len_col, column(gemit[s]), 0.0)
            weight = (gblank + gemit_col) * scale[s]
        else:
            weight = gblank * scale[s]
        grad = jnp.where(lane_v == 0, gblank, 0.0) - scores_s[s] * weight
        if s < S - 1:
            grad = grad + jnp.where(lane_v == next_label[s], gemit_col, 0.0)
        bias_total = bias_total + jnp.sum(grad, axis=0, keepdims=True)
        low_s[s * rows : (s + 1) * rows, :] = grad.astype(BF16)

    grad_enc_proj = jnp.zeros((rows, w_enc_ref.shape[1]), F32)
    grad_pred_proj = jnp.zeros((places, w_pred_ref.shape[1]), F32)
    for s in range(S):
        grad_hidden = jnp.dot(
            low_s[s * rows : (s + 1) * rows, :], w_joint_s[...], preferred_element_type=F32
        )
        active = active_s[s]
        grad_pre = grad_hidden * (1.0 - active * active)
        grad_enc_proj = grad_enc_proj + grad_pre
        grad_pred_proj = grad_pred_proj + over_rows(picks_s[s], grad_pre.astype(BF16))
    bias_s[...] = bias_total
    grad_enc_s[...] = grad_enc_proj.astype(BF16)
    grad_pred_s[...] = grad_pred_proj.astype(BF16)

    core = lax.axis_index("c")
    half = width // 2
    for out_ref, which in ((send_ref, 1 - core), (keep_ref, core)):
        columns = pl.ds(pl.multiple_of(which * half, half), half)
        products = (
            over_rows(enc_ref[...], grad_enc_s[:, columns]),
            over_rows(pred_s[...], grad_pred_s[:, columns]),
            over_rows(low_s[...], hidden_s[:, columns]),
        )
        at = 0
        for product in products:
            for j in range(half // 128):
                out_ref[at : at + width, :] = product[:, j * 128 : (j + 1) * 128]
                at += width
        base = at - (half // 128) * width + vocab
        for j in range(half // 128):
            lanes = pl.ds(pl.multiple_of(which * half + j * 128, 128), 128)
            out_ref[base + j * width : base + j * width + 1, :] = bias_s[:, lanes]
            out_ref[base + j * width + 1 : base + j * width + 2, :] = jnp.broadcast_to(loss, (1, 128))


def local_grads(
    encoder_out, predictor_out, w_encoder, w_predictor, w_joint, joint_bias,
    labels, frame_lens, label_lens, prune_starts,
):
    count, frames, enc_width = encoder_out.shape
    pred_width = predictor_out.shape[2]
    joint_width, vocab = w_joint.shape
    rows = count * frames
    width = -(-vocab // 128) * 128
    places = 128
    vmem = pl.BlockSpec(memory_space=pltpu.VMEM)
    return pl.pallas_call(
        joint_kernel,
        out_shape=(pltpu.VMEM((3 * width * width // 256, 128), F32),) * 2,
        in_specs=[pl.BlockSpec(memory_space=pltpu.HBM)] * 10,
        out_specs=(vmem, vmem),
        scratch_shapes=[
            pltpu.SMEM((count,), jnp.int32),
            pltpu.SMEM((count,), jnp.int32),
            pltpu.VMEM((rows, enc_width), BF16),
            pltpu.VMEM((predictor_out.shape[1], count, pred_width), BF16),
            pltpu.VMEM(w_encoder.shape, BF16),
            pltpu.VMEM(w_predictor.shape, BF16),
            pltpu.VMEM((vocab, joint_width), BF16),
            pltpu.VMEM((1, vocab), F32),
            pltpu.VMEM(labels.shape, jnp.int32),
            pltpu.VMEM(prune_starts.shape, jnp.int32),
            pltpu.SemaphoreType.DMA((10,)),
            pltpu.VMEM((places, pred_width), BF16),
            pltpu.VMEM((width, joint_width), BF16),
            pltpu.VMEM((1, width), F32),
            pltpu.VMEM((S, rows, joint_width), F32),
            pltpu.VMEM((S * rows, joint_width), BF16),
            pltpu.VMEM((S, rows, width), F32),
            pltpu.VMEM((S * rows, width), BF16),
            pltpu.VMEM((S, rows, places), BF16),
            pltpu.VMEM((S, frames, 128), F32),
            pltpu.VMEM((S - 1, frames, 128), F32),
            pltpu.VMEM((frames, 128), jnp.int32),
            pltpu.VMEM((len(PAIRS), frames, 128), F32),
            pltpu.VMEM((S, frames, 128), F32),
            pltpu.VMEM((S, frames, 128), F32),
            pltpu.VMEM((S, frames, 128), F32),
            pltpu.VMEM((rows, joint_width), BF16),
            pltpu.VMEM((places, joint_width), BF16),
        ],
        compiler_params=pltpu.CompilerParams(vmem_limit_bytes=56 * 2**20),
        name="joint",
    )(
        frame_lens, label_lens, encoder_out.reshape(rows, enc_width),
        jnp.swapaxes(predictor_out, 0, 1),        w_encoder, w_predictor, w_joint.T, joint_bias.reshape(1, vocab), labels, prune_starts,
    )


def unpack_kernel(utterances, mine_ref, other_ref, enc_ref, pred_ref, joint_ref, bias_ref, loss_ref):
    core = lax.axis_index("c")
    width = enc_ref.shape[0]
    vocab = joint_ref.shape[0]
    half = width // 256

    def place(refs):
        for h in range(2):
            for m, out_ref in enumerate((enc_ref, pred_ref, joint_ref)):
                for j in range(half):
                    at = (m * half + j) * width
                    lane = (h * half + j) * 128
                    size = out_ref.shape[0]
                    out_ref[:, lane : lane + 128] = refs[h][at : at + size, :]
            for j in range(half):
                at = (2 * half + j) * width + vocab
                lane = (h * half + j) * 128
                size = min(128, vocab - lane)
                bias_ref[:, lane : lane + size] = refs[h][at : at + 1, :size]
        at = 2 * half * width + vocab + 1
        loss_ref[...] = refs[0][at : at + 1, 0:1] / utterances

    @pl.when(core == 0)
    def _():
        place((mine_ref, other_ref))

    @pl.when(core != 0)
    def _():
        place((other_ref, mine_ref))


def merge_kernel(keep_ref, recv_ref, out_ref):
    out_ref[...] = keep_ref[...] + recv_ref[...]

    @pl.when(lax.axis_index("c") == SECOND)
    def _():
        spare = out_ref.shape[0] - 8
        first = out_ref[spare:, :]
        out_ref[spare:, :] = lax.fori_loop(0, STAGGER, lambda _, v: jnp.tanh(v), first)


def merge(keep, recv):
    vmem = pl.BlockSpec(memory_space=pltpu.VMEM)
    return pl.pallas_call(
        merge_kernel,
        out_shape=pltpu.VMEM(keep.shape, F32),
        in_specs=[vmem, vmem],
        out_specs=vmem,
        input_output_aliases={0: 0},
        compiler_params=pltpu.CompilerParams(vmem_limit_bytes=8 * 2**20),
        name="merge",
    )(keep, recv)


def swap_cores(value):
    return lax.ppermute(value, "c", [(0, 1), (1, 0)])


def sum_at_owner(value, axes):
    members = lax.axis_size(axes)
    arrived = lax.all_to_all(value, axes, split_axis=0, concat_axis=0, tiled=True)
    return arrived.reshape(members, -1, value.shape[1]).sum(axis=0)


def from_all(value, axes):
    members = lax.axis_size(axes)
    spread = jnp.broadcast_to(value[None], (members, *value.shape))
    spread = spread.reshape(-1, value.shape[1])
    return lax.all_to_all(spread, axes, split_axis=0, concat_axis=0, tiled=True)


def sum_everywhere(value, axes):
    sizes = [lax.axis_size(a) for a in axes]
    assert sizes == [2, 2]
    arrived = []
    for step in (2, 1, 3):
        pairs = [
            (2 * (n % 2) + n // 2, 2 * ((n + step) % 4 % 2) + (n + step) % 4 // 2)
            for n in range(4)
        ]
        arrived.append(lax.ppermute(value, axes, pairs))
    return (value + arrived[0]) + (arrived[1] + arrived[2])


def shards(*args):
    keep, send = local_grads(*args)
    mine = merge(keep, swap_cores(send))
    mine = sum_at_owner(mine, NEAR)
    mine = sum_everywhere(mine, FAR)
    mine = from_all(mine, NEAR)
    other = swap_cores(mine)
    width, vocab = args[4].shape
    utterances = args[0].shape[0] * lax.axis_size(AXES)
    vmem = pl.BlockSpec(memory_space=pltpu.VMEM)
    grad_encoder, grad_predictor, grad_joint, grad_bias, loss = pl.pallas_call(
        functools.partial(unpack_kernel, utterances),
        out_shape=(
            jax.ShapeDtypeStruct((width, width), F32),
            jax.ShapeDtypeStruct((width, width), F32),
            jax.ShapeDtypeStruct((vocab, width), F32),
            jax.ShapeDtypeStruct((1, vocab), F32),
            jax.ShapeDtypeStruct((1, 1), F32),
        ),
        in_specs=[vmem, vmem],
        out_specs=(vmem,) * 5,
        compiler_params=pltpu.CompilerParams(vmem_limit_bytes=20 * 2**20),
        name="unpack",
    )(mine, other)
    return grad_encoder, grad_predictor, grad_joint.T, grad_bias.reshape(vocab), loss.reshape(())


def solution(mesh):
    mesh = jax.sharding.Mesh(mesh.devices.reshape(2, 2, 4, 4, 2, 2), AXES)
    in_specs = (
        P(AXES, None, None), P(AXES, None, None), P(), P(), P(), P(),
        P(AXES, None), P(AXES), P(AXES), P(AXES, None),
    )
    return jax.shard_map(
        shards, mesh=mesh, in_specs=in_specs, out_specs=(P(),) * 5, check_vma=False
    )
```

```python
import functools

import jax
import jax.numpy as jnp
from jax import lax
from jax.experimental import pallas as pl
from jax.experimental.pallas import tpu as pltpu
from jax.sharding import PartitionSpec as P

S = 5
NEG_FILL = -10000.0
LOW = -1e30
F32 = jnp.float32
BF16 = jnp.bfloat16
AXES = ("zq", "zp", "x", "y", "zh", "c")
NEAR = ("zp", "x", "y")
FAR = ("zq", "zh")
SECOND = 0
STAGGER = 900
PAIRS = tuple((j, s) for s in range(S) for j in range(s + 1))


def over_rows(a, b):
    return lax.dot_general(a, b, (((0,), (0,)), ((), ())), preferred_element_type=F32)


def per_utterance(index, values):
    out = jnp.where(index == 0, values[0], values[-1])
    for b in range(1, len(values) - 1):
        out = jnp.where(index == b, values[b], out)
    return out


def shifted(rows, amount, lowest, fill):
    width = len(rows)
    span = {i: rows[i] if 0 <= i < width else fill for i in range(lowest, width + lowest + 7)}
    bits = amount - lowest
    for bit in (4, 2, 1):
        on = (bits & bit) != 0
        top = max(span)
        span = {
            i: jnp.where(on, span[i + bit], span[i])
            for i in span
            if i + bit <= top
        }
    return [span[s + lowest] for s in range(width)]


def joint_kernel(
    frames_hbm, lens_hbm, enc_hbm, pred_hbm, w_enc_hbm, w_pred_hbm, w_joint_hbm,
    bias_hbm, labels_hbm, starts_hbm,
    keep_ref, send_ref,
    frames_ref, lens_ref, enc_ref, pred_ref, w_enc_ref, w_pred_ref, w_joint_ref,
    bias_ref, labels_ref, starts_ref, load_sems,
    pred_s, w_joint_s, bias_s, active_s, hidden_s, scores_s, low_s, picks_s,
    blank_s, emit_s, shift_s, terms_s, sums_s, state_s, gblank_s, grad_enc_s, grad_pred_s,
):
    loads = {
        name: pltpu.make_async_copy(src, dst, load_sems.at[i])
        for i, (name, src, dst) in enumerate((
            ("starts", starts_hbm, starts_ref),
            ("frames", frames_hbm, frames_ref),
            ("lens", lens_hbm, lens_ref),
            ("enc", enc_hbm, enc_ref),
            ("w_enc", w_enc_hbm, w_enc_ref),
            ("pred", pred_hbm, pred_ref),
            ("w_pred", w_pred_hbm, w_pred_ref),
            ("labels", labels_hbm, labels_ref),
            ("bias", bias_hbm, bias_ref),
            ("w_joint", w_joint_hbm, w_joint_ref),
        ))
    }
    for load in loads.values():
        load.start()

    row_count, count, _ = pred_ref.shape
    vocab = w_joint_ref.shape[0]
    slots = labels_ref.shape[1]
    rows = enc_ref.shape[0]
    frames = rows // count
    width = w_joint_s.shape[0]
    places = pred_s.shape[0]

    pred_s[...] = jnp.zeros_like(pred_s)
    last = (width // 128 - 1) * 128
    w_joint_s[last:, :] = jnp.zeros((128, w_joint_s.shape[1]), BF16)
    bias_s[...] = jnp.full_like(bias_s, LOW)
    for name in ("starts", "frames", "lens"):
        loads[name].wait()
    frame_len = [frames_ref[b] for b in range(count)]
    label_len = [lens_ref[b] for b in range(count)]

    eye = lax.broadcasted_iota(jnp.int32, (frames, frames), 0) == lax.broadcasted_iota(
        jnp.int32, (frames, frames), 1
    )
    starts_f = starts_ref[...].astype(F32)
    lane_b = lax.broadcasted_iota(jnp.int32, (frames, 128), 1)
    start_cols = []
    start_tb = jnp.zeros((frames, 128), F32)
    for b in range(count):
        line = jnp.broadcast_to(starts_f[b : b + 1, :], (frames, frames))
        col = jnp.sum(jnp.where(eye, line, 0.0), axis=1, keepdims=True)
        start_cols.append(col)
        start_tb = jnp.where(lane_b == b, col, start_tb)
    start_col = jnp.concatenate(start_cols, axis=0).astype(jnp.int32)
    start_tb = start_tb.astype(jnp.int32)
    row_b = lax.broadcasted_iota(jnp.int32, (rows, 1), 0) // frames
    label_len_col = per_utterance(row_b, label_len)
    label_len_row = per_utterance(lax.broadcasted_iota(jnp.int32, (1, 128), 1), label_len)
    frame_len_row = per_utterance(lax.broadcasted_iota(jnp.int32, (1, 128), 1), frame_len)
    shift_s[0:1, :] = jnp.zeros((1, 128), jnp.int32)
    shift_s[1:frames, :] = start_tb[1:, :] - start_tb[:-1, :]

    for name in ("enc", "w_enc", "pred", "w_pred"):
        loads[name].wait()
    for u in range(row_count):
        pred_s[u * count : (u + 1) * count, :] = pred_ref[u]
    enc_proj = jnp.dot(enc_ref[...], w_enc_ref[...], preferred_element_type=F32).astype(BF16)
    enc_proj = enc_proj.astype(F32)
    pred_proj = jnp.dot(pred_s[...], w_pred_ref[...], preferred_element_type=F32).astype(BF16)

    for name in ("labels", "bias", "w_joint"):
        loads[name].wait()
    w_joint_s[:vocab, :] = w_joint_ref[...]
    bias_s[:, :vocab] = bias_ref[...]
    lane_u = lax.broadcasted_iota(jnp.int32, (rows, places), 1)
    lane_k = lax.broadcasted_iota(jnp.int32, (rows, slots), 1)
    label_rows = jnp.concatenate(
        [jnp.broadcast_to(labels_ref[b : b + 1, :].astype(F32), (frames, slots)) for b in range(count)],
        axis=0,
    )
    lane_v = lax.broadcasted_iota(jnp.int32, (rows, width), 1)
    next_label, scale = [], []
    for s in range(S):
        pos = start_col + s
        pick = (lane_u == pos * count + row_b).astype(F32).astype(BF16)
        picks_s[s] = pick
        picked = jnp.dot(pick, pred_proj, preferred_element_type=F32)
        active = jnp.tanh(enc_proj + picked)
        active_s[s] = active
        hidden = active.astype(BF16)
        hidden_s[s * rows : (s + 1) * rows, :] = hidden
        logits = lax.dot_general(
            hidden, w_joint_s[...], (((1,), (1,)), ((), ())), preferred_element_type=F32
        )
        logits = logits + bias_s[...]
        peak = jnp.max(logits, axis=1, keepdims=True)
        raised = jnp.exp(logits - peak)
        scores_s[s] = raised
        total = jnp.sum(raised, axis=1, keepdims=True)
        norm = peak + jnp.log(total)
        scale.append(1.0 / total)
        blank = jnp.where(pos <= label_len_col, logits[:, 0:1] - norm, NEG_FILL)
        blank_tb = jnp.zeros((frames, 128), F32)
        for b in range(count):
            blank_tb = jnp.where(lane_b == b, blank[b * frames : (b + 1) * frames, :], blank_tb)
        blank_s[s] = blank_tb
        if s < S - 1:
            label = jnp.sum(
                jnp.where(lane_k == pos, label_rows, 0.0), axis=1, keepdims=True
            ).astype(jnp.int32)
            next_label.append(label)
            emit = jnp.sum(jnp.where(lane_v == label, logits, 0.0), axis=1, keepdims=True)
            emit = jnp.where(pos < label_len_col, emit - norm, NEG_FILL)
            emit_tb = jnp.zeros((frames, 128), F32)
            for b in range(count):
                emit_tb = jnp.where(lane_b == b, emit[b * frames : (b + 1) * frames, :], emit_tb)
            emit_s[s] = emit_tb

    fill = jnp.full((1, 128), NEG_FILL, F32)
    state = None
    for t in range(frames):
        if t == 0:
            entering = [jnp.zeros((1, 128), F32)] + [fill] * (S - 1)
        else:
            leaving = [state[s] + blank_s[s, t - 1 : t, :] for s in range(S)]
            entering = shifted(leaving, shift_s[t : t + 1, :], -3, fill)
        emits = [emit_s[s, t : t + 1, :] for s in range(S - 1)]
        updated = []
        for s in range(S):
            routes = []
            for j in range(s + 1):
                way = entering[j]
                for i in range(j, s):
                    way = way + emits[i]
                routes.append(way)
            best = routes[0]
            for r in routes[1:]:
                best = jnp.maximum(best, r)
            terms = [jnp.exp(r - best) for r in routes]
            total = terms[0]
            for r in terms[1:]:
                total = total + r
            for j in range(s + 1):
                terms_s[PAIRS.index((j, s)), t : t + 1, :] = terms[j]
            sums_s[s, t : t + 1, :] = total
            updated.append(best + jnp.log(total))
        if t == 0:
            state = updated
        else:
            live = t < frame_len_row
            state = [jnp.where(live, n, o) for n, o in zip(updated, state)]

    frame_tb = lax.broadcasted_iota(jnp.int32, (frames, 128), 0)
    ending = frame_tb == frame_len_row - 1
    valid = lax.broadcasted_iota(jnp.int32, (1, 128), 1) < count
    final_start = jnp.sum(jnp.where(ending, start_tb.astype(F32), 0.0), axis=0, keepdims=True)
    final_pos = label_len_row - final_start.astype(jnp.int32)
    share = jnp.where(valid, -1.0 / frame_len_row.astype(F32), 0.0)
    likelihood = jnp.zeros((1, 128), F32)
    grads = []
    for s in range(S):
        here = final_pos == s
        end_blank = jnp.sum(jnp.where(ending, blank_s[s], 0.0), axis=0, keepdims=True)
        likelihood = jnp.where(here, state[s] + end_blank, likelihood)
        grads.append(jnp.where(here, share, 0.0))
        gblank_s[s] = jnp.where(ending & here, share, 0.0)
    loss = jnp.sum(jnp.where(valid, likelihood * share, 0.0), axis=1, keepdims=True)

    for s in range(S):
        inverse = 1.0 / sums_s[s]
        for j in range(s + 1):
            terms_s[PAIRS.index((j, s))] = terms_s[PAIRS.index((j, s))] * inverse

    none = jnp.zeros((1, 128), F32)
    for t in range(frames - 1, 0, -1):
        live = t < frame_len_row
        for s in range(S):
            state_s[s, t : t + 1, :] = jnp.where(live, grads[s], 0.0)
        back = []
        for j in range(S):
            parts = [grads[s] * terms_s[PAIRS.index((j, s)), t : t + 1, :] for s in range(j, S)]
            total = parts[0]
            for r in parts[1:]:
                total = total + r
            back.append(total)
        earlier = shifted(back, -shift_s[t : t + 1, :], -3, none)
        for s in range(S):
            gblank_s[s, t - 1 : t, :] += jnp.where(live, earlier[s], 0.0)
        grads = [jnp.where(live, n, o) for n, o in zip(earlier, grads)]
    for s in range(S):
        state_s[s, 0:1, :] = grads[s]

    def column(table):
        return jnp.concatenate([table[:, b : b + 1] for b in range(count)], axis=0)

    gemit = [jnp.zeros((frames, 128), F32) for _ in range(S - 1)]
    for j, s in PAIRS:
        if j < s:
            flow = state_s[s] * terms_s[PAIRS.index((j, s))]
            for i in range(j, s):
                gemit[i] = gemit[i] + flow
    bias_total = jnp.zeros((1, width), F32)
    for s in range(S):
        pos = start_col + s
        gblank = jnp.where(pos <= label_len_col, column(gblank_s[s]), 0.0)
        if s < S - 1:
            gemit_col = jnp.where(pos < label_len_col, column(gemit[s]), 0.0)
            weight = (gblank + gemit_col) * scale[s]
        else:
            weight = gblank * scale[s]
        grad = jnp.where(lane_v == 0, gblank, 0.0) - scores_s[s] * weight
        if s < S - 1:
            grad = grad + jnp.where(lane_v == next_label[s], gemit_col, 0.0)
        bias_total = bias_total + jnp.sum(grad, axis=0, keepdims=True)
        low_s[s * rows : (s + 1) * rows, :] = grad.astype(BF16)

    grad_enc_proj = jnp.zeros((rows, w_enc_ref.shape[1]), F32)
    grad_pred_proj = jnp.zeros((places, w_pred_ref.shape[1]), F32)
    for s in range(S):
        grad_hidden = jnp.dot(
            low_s[s * rows : (s + 1) * rows, :], w_joint_s[...], preferred_element_type=F32
        )
        active = active_s[s]
        grad_pre = grad_hidden * (1.0 - active * active)
        grad_enc_proj = grad_enc_proj + grad_pre
        grad_pred_proj = grad_pred_proj + over_rows(picks_s[s], grad_pre.astype(BF16))
    bias_s[...] = bias_total
    grad_enc_s[...] = grad_enc_proj.astype(BF16)
    grad_pred_s[...] = grad_pred_proj.astype(BF16)

    core = lax.axis_index("c")
    half = width // 2
    for out_ref, which in ((send_ref, 1 - core), (keep_ref, core)):
        columns = pl.ds(pl.multiple_of(which * half, half), half)
        products = (
            over_rows(enc_ref[...], grad_enc_s[:, columns]),
            over_rows(pred_s[...], grad_pred_s[:, columns]),
            over_rows(low_s[...], hidden_s[:, columns]),
        )
        at = 0
        for product in products:
            for j in range(half // 128):
                out_ref[at : at + width, :] = product[:, j * 128 : (j + 1) * 128]
                at += width
        base = at - (half // 128) * width + vocab
        for j in range(half // 128):
            lanes = pl.ds(pl.multiple_of(which * half + j * 128, 128), 128)
            out_ref[base + j * width : base + j * width + 1, :] = bias_s[:, lanes]
            out_ref[base + j * width + 1 : base + j * width + 2, :] = jnp.broadcast_to(loss, (1, 128))


def local_grads(
    encoder_out, predictor_out, w_encoder, w_predictor, w_joint, joint_bias,
    labels, frame_lens, label_lens, prune_starts,
):
    count, frames, enc_width = encoder_out.shape
    pred_width = predictor_out.shape[2]
    joint_width, vocab = w_joint.shape
    rows = count * frames
    width = -(-vocab // 128) * 128
    places = 128
    vmem = pl.BlockSpec(memory_space=pltpu.VMEM)
    return pl.pallas_call(
        joint_kernel,
        out_shape=(pltpu.VMEM((3 * width * width // 256, 128), F32),) * 2,
        in_specs=[pl.BlockSpec(memory_space=pltpu.HBM)] * 10,
        out_specs=(vmem, vmem),
        scratch_shapes=[
            pltpu.SMEM((count,), jnp.int32),
            pltpu.SMEM((count,), jnp.int32),
            pltpu.VMEM((rows, enc_width), BF16),
            pltpu.VMEM((predictor_out.shape[1], count, pred_width), BF16),
            pltpu.VMEM(w_encoder.shape, BF16),
            pltpu.VMEM(w_predictor.shape, BF16),
            pltpu.VMEM((vocab, joint_width), BF16),
            pltpu.VMEM((1, vocab), F32),
            pltpu.VMEM(labels.shape, jnp.int32),
            pltpu.VMEM(prune_starts.shape, jnp.int32),
            pltpu.SemaphoreType.DMA((10,)),
            pltpu.VMEM((places, pred_width), BF16),
            pltpu.VMEM((width, joint_width), BF16),
            pltpu.VMEM((1, width), F32),
            pltpu.VMEM((S, rows, joint_width), F32),
            pltpu.VMEM((S * rows, joint_width), BF16),
            pltpu.VMEM((S, rows, width), F32),
            pltpu.VMEM((S * rows, width), BF16),
            pltpu.VMEM((S, rows, places), BF16),
            pltpu.VMEM((S, frames, 128), F32),
            pltpu.VMEM((S - 1, frames, 128), F32),
            pltpu.VMEM((frames, 128), jnp.int32),
            pltpu.VMEM((len(PAIRS), frames, 128), F32),
            pltpu.VMEM((S, frames, 128), F32),
            pltpu.VMEM((S, frames, 128), F32),
            pltpu.VMEM((S, frames, 128), F32),
            pltpu.VMEM((rows, joint_width), BF16),
            pltpu.VMEM((places, joint_width), BF16),
        ],
        compiler_params=pltpu.CompilerParams(vmem_limit_bytes=56 * 2**20),
        name="joint",
    )(
        frame_lens, label_lens, encoder_out.reshape(rows, enc_width),
        jnp.swapaxes(predictor_out, 0, 1),        w_encoder, w_predictor, w_joint.T, joint_bias.reshape(1, vocab), labels, prune_starts,
    )


def place_kernel(utterances, sides, *refs):
    half_ref, others = refs[0], refs[1:]
    enc_ref, pred_ref, joint_ref, bias_ref, loss_ref, sems = others[-6:]
    core = lax.axis_index("c")
    width = enc_ref.shape[0]
    vocab = joint_ref.shape[0]
    tiles = width // 256
    outs = (enc_ref, pred_ref, joint_ref)

    def place(h):
        copies = []
        for m, out_ref in enumerate(outs):
            size = out_ref.shape[0]
            for j in range(tiles):
                lane = (h * tiles + j) * 128
                copies.append(
                    pltpu.make_async_copy(
                        half_ref.at[pl.ds((m * tiles + j) * width, size), :],
                        out_ref.at[:, pl.ds(lane, 128)],
                        sems.at[m * tiles + j],
                    )
                )
        for copy in copies:
            copy.start()
        if sides:
            bias_ref[...] = others[3][...]
        for j in range(tiles):
            at = (2 * tiles + j) * width + vocab
            lane = (h * tiles + j) * 128
            size = min(128, vocab - lane)
            bias_ref[:, lane : lane + size] = half_ref[at : at + 1, :size]
        at = 2 * tiles * width + vocab + 1
        loss_ref[...] = half_ref[at : at + 1, 0:1] / utterances
        for copy in copies:
            copy.wait()

    for h in range(2):
        @pl.when((core + sides) % 2 == h)
        def _():
            place(h)


def place(half, so_far, utterances, shapes):
    vmem = pl.BlockSpec(memory_space=pltpu.VMEM)
    hbm = pl.BlockSpec(memory_space=pltpu.HBM)
    big, small = shapes[:3], shapes[3:]
    out_shape = [pltpu.HBM(d, F32) for d in big] + [jax.ShapeDtypeStruct(d, F32) for d in small]
    inputs = (half, *so_far[:4])
    return pl.pallas_call(
        functools.partial(place_kernel, utterances, int(bool(so_far))),
        out_shape=out_shape,
        in_specs=[vmem] + ([hbm] * 3 + [vmem] if so_far else []),
        out_specs=[hbm] * 3 + [vmem] * 2,
        scratch_shapes=[pltpu.SemaphoreType.DMA((6,))],
        input_output_aliases={1: 0, 2: 1, 3: 2} if so_far else {},
        compiler_params=pltpu.CompilerParams(vmem_limit_bytes=8 * 2**20),
        cost_estimate=pl.CostEstimate(
            flops=2**24, bytes_accessed=2 * half.size * 4, transcendentals=0
        ),
        name="place",
    )(*inputs)


def merge_kernel(keep_ref, recv_ref, out_ref):
    out_ref[...] = keep_ref[...] + recv_ref[...]

    @pl.when(lax.axis_index("c") == SECOND)
    def _():
        spare = out_ref.shape[0] - 8
        first = out_ref[spare:, :]
        out_ref[spare:, :] = lax.fori_loop(0, STAGGER, lambda _, v: jnp.tanh(v), first)


def merge(keep, recv):
    vmem = pl.BlockSpec(memory_space=pltpu.VMEM)
    return pl.pallas_call(
        merge_kernel,
        out_shape=pltpu.VMEM(keep.shape, F32),
        in_specs=[vmem, vmem],
        out_specs=vmem,
        input_output_aliases={0: 0},
        compiler_params=pltpu.CompilerParams(vmem_limit_bytes=8 * 2**20),
        name="merge",
    )(keep, recv)


def swap_cores(value):
    return lax.ppermute(value, "c", [(0, 1), (1, 0)])


def sum_at_owner(value, axes):
    members = lax.axis_size(axes)
    arrived = lax.all_to_all(value, axes, split_axis=0, concat_axis=0, tiled=True)
    return arrived.reshape(members, -1, value.shape[1]).sum(axis=0)


def from_all(value, axes):
    members = lax.axis_size(axes)
    spread = jnp.broadcast_to(value[None], (members, *value.shape))
    spread = spread.reshape(-1, value.shape[1])
    return lax.all_to_all(spread, axes, split_axis=0, concat_axis=0, tiled=True)


def sum_everywhere(value, axes):
    sizes = [lax.axis_size(a) for a in axes]
    assert sizes == [2, 2]
    arrived = []
    for step in (2, 1, 3):
        pairs = [
            (2 * (n % 2) + n // 2, 2 * ((n + step) % 4 % 2) + (n + step) % 4 // 2)
            for n in range(4)
        ]
        arrived.append(lax.ppermute(value, axes, pairs))
    return (value + arrived[0]) + (arrived[1] + arrived[2])


def shards(*args):
    keep, send = local_grads(*args)
    mine = merge(keep, swap_cores(send))
    mine = sum_at_owner(mine, NEAR)
    mine = sum_everywhere(mine, FAR)
    mine = from_all(mine, NEAR)
    other = swap_cores(mine)
    width, vocab = args[4].shape
    utterances = args[0].shape[0] * lax.axis_size(AXES)
    shapes = ((width, width), (width, width), (vocab, width), (1, vocab), (1, 1))
    so_far = place(mine, (), utterances, shapes)
    grad_encoder, grad_predictor, grad_joint, grad_bias, loss = place(
        other, so_far, utterances, shapes
    )
    return grad_encoder, grad_predictor, grad_joint.T, grad_bias.reshape(vocab), loss.reshape(())


def solution(mesh):
    mesh = jax.sharding.Mesh(mesh.devices.reshape(2, 2, 4, 4, 2, 2), AXES)
    in_specs = (
        P(AXES, None, None), P(AXES, None, None), P(), P(), P(), P(),
        P(AXES, None), P(AXES), P(AXES), P(AXES, None),
    )
    return jax.shard_map(
        shards, mesh=mesh, in_specs=in_specs, out_specs=(P(),) * 5, check_vma=False
    )
```

```python
import functools

import jax
import jax.numpy as jnp
from jax import lax
from jax.experimental import pallas as pl
from jax.experimental.pallas import tpu as pltpu
from jax.sharding import PartitionSpec as P

S = 5
NEG_FILL = -10000.0
LOW = -1e30
F32 = jnp.float32
BF16 = jnp.bfloat16
AXES = ("zq", "zp", "x", "y", "zh", "c")
NEAR = ("zp", "x", "y")
FAR = ("zq", "zh")
SECOND = 0
STAGGER = 750
PAIRS = tuple((j, s) for s in range(S) for j in range(s + 1))


def tree(op, terms):
    while len(terms) > 1:
        pairs = [op(a, b) for a, b in zip(terms[::2], terms[1::2])]
        terms = pairs + terms[len(terms) // 2 * 2 :]
    return terms[0]


def over_rows(a, b):
    return lax.dot_general(a, b, (((0,), (0,)), ((), ())), preferred_element_type=F32)


def per_utterance(index, values):
    out = jnp.where(index == 0, values[0], values[-1])
    for b in range(1, len(values) - 1):
        out = jnp.where(index == b, values[b], out)
    return out


def shifted(rows, amount, lowest, fill):
    width = len(rows)
    span = {i: rows[i] if 0 <= i < width else fill for i in range(lowest, width + lowest + 7)}
    bits = amount - lowest
    for bit in (4, 2, 1):
        on = (bits & bit) != 0
        top = max(span)
        span = {
            i: jnp.where(on, span[i + bit], span[i])
            for i in span
            if i + bit <= top
        }
    return [span[s + lowest] for s in range(width)]


def joint_kernel(
    frames_hbm, lens_hbm, enc_hbm, pred_hbm, w_enc_hbm, w_pred_hbm, w_joint_hbm,
    bias_hbm, labels_hbm, starts_hbm,
    keep_ref, send_ref,
    frames_ref, lens_ref, enc_ref, pred_ref, w_enc_ref, w_pred_ref, w_joint_ref,
    bias_ref, labels_ref, starts_ref, load_sems,
    pred_s, w_joint_s, bias_s, active_s, hidden_s, scores_s, low_s, picks_s,
    blank_s, emit_s, shift_s, terms_s, sums_s, state_s, gblank_s, grad_enc_s, grad_pred_s,
):
    loads = {
        name: pltpu.make_async_copy(src, dst, load_sems.at[i])
        for i, (name, src, dst) in enumerate((
            ("starts", starts_hbm, starts_ref),
            ("frames", frames_hbm, frames_ref),
            ("lens", lens_hbm, lens_ref),
            ("enc", enc_hbm, enc_ref),
            ("w_enc", w_enc_hbm, w_enc_ref),
            ("pred", pred_hbm, pred_ref),
            ("w_pred", w_pred_hbm, w_pred_ref),
            ("labels", labels_hbm, labels_ref),
            ("bias", bias_hbm, bias_ref),
            ("w_joint", w_joint_hbm, w_joint_ref),
        ))
    }
    for load in loads.values():
        load.start()

    row_count, count, _ = pred_ref.shape
    vocab = w_joint_ref.shape[0]
    slots = labels_ref.shape[1]
    rows = enc_ref.shape[0]
    frames = rows // count
    width = w_joint_s.shape[0]
    places = pred_s.shape[0]

    pred_s[...] = jnp.zeros_like(pred_s)
    last = (width // 128 - 1) * 128
    w_joint_s[last:, :] = jnp.zeros((128, w_joint_s.shape[1]), BF16)
    bias_s[...] = jnp.full_like(bias_s, LOW)
    for name in ("starts", "frames", "lens"):
        loads[name].wait()
    frame_len = [frames_ref[b] for b in range(count)]
    label_len = [lens_ref[b] for b in range(count)]

    eye = lax.broadcasted_iota(jnp.int32, (frames, frames), 0) == lax.broadcasted_iota(
        jnp.int32, (frames, frames), 1
    )
    starts_f = starts_ref[...].astype(F32)
    lane_b = lax.broadcasted_iota(jnp.int32, (frames, 128), 1)
    start_cols = []
    start_tb = jnp.zeros((frames, 128), F32)
    for b in range(count):
        line = jnp.broadcast_to(starts_f[b : b + 1, :], (frames, frames))
        col = jnp.sum(jnp.where(eye, line, 0.0), axis=1, keepdims=True)
        start_cols.append(col)
        start_tb = jnp.where(lane_b == b, col, start_tb)
    start_col = jnp.concatenate(start_cols, axis=0).astype(jnp.int32)
    start_tb = start_tb.astype(jnp.int32)
    row_b = lax.broadcasted_iota(jnp.int32, (rows, 1), 0) // frames
    label_len_col = per_utterance(row_b, label_len)
    label_len_row = per_utterance(lax.broadcasted_iota(jnp.int32, (1, 128), 1), label_len)
    frame_len_row = per_utterance(lax.broadcasted_iota(jnp.int32, (1, 128), 1), frame_len)
    shift_s[0:1, :] = jnp.zeros((1, 128), jnp.int32)
    shift_s[1:frames, :] = start_tb[1:, :] - start_tb[:-1, :]

    for name in ("enc", "w_enc", "pred", "w_pred"):
        loads[name].wait()
    for u in range(row_count):
        pred_s[u * count : (u + 1) * count, :] = pred_ref[u]
    enc_proj = jnp.dot(enc_ref[...], w_enc_ref[...], preferred_element_type=F32).astype(BF16)
    enc_proj = enc_proj.astype(F32)
    pred_proj = jnp.dot(pred_s[...], w_pred_ref[...], preferred_element_type=F32).astype(BF16)

    for name in ("labels", "bias", "w_joint"):
        loads[name].wait()
    w_joint_s[:vocab, :] = w_joint_ref[...]
    bias_s[:, :vocab] = bias_ref[...]
    lane_u = lax.broadcasted_iota(jnp.int32, (rows, places), 1)
    lane_k = lax.broadcasted_iota(jnp.int32, (rows, slots), 1)
    label_rows = jnp.concatenate(
        [jnp.broadcast_to(labels_ref[b : b + 1, :].astype(F32), (frames, slots)) for b in range(count)],
        axis=0,
    )
    lane_v = lax.broadcasted_iota(jnp.int32, (rows, width), 1)
    next_label, scale = [], []
    for s in range(S):
        pos = start_col + s
        pick = (lane_u == pos * count + row_b).astype(F32).astype(BF16)
        picks_s[s] = pick
        picked = jnp.dot(pick, pred_proj, preferred_element_type=F32)
        active = jnp.tanh(enc_proj + picked)
        active_s[s] = active
        hidden = active.astype(BF16)
        hidden_s[s * rows : (s + 1) * rows, :] = hidden
        logits = lax.dot_general(
            hidden, w_joint_s[...], (((1,), (1,)), ((), ())), preferred_element_type=F32
        )
        logits = logits + bias_s[...]
        peak = jnp.max(logits, axis=1, keepdims=True)
        raised = jnp.exp(logits - peak)
        scores_s[s] = raised
        total = jnp.sum(raised, axis=1, keepdims=True)
        norm = peak + jnp.log(total)
        scale.append(1.0 / total)
        blank = jnp.where(pos <= label_len_col, logits[:, 0:1] - norm, NEG_FILL)
        blank_tb = jnp.zeros((frames, 128), F32)
        for b in range(count):
            blank_tb = jnp.where(lane_b == b, blank[b * frames : (b + 1) * frames, :], blank_tb)
        blank_s[s] = blank_tb
        if s < S - 1:
            label = jnp.sum(
                jnp.where(lane_k == pos, label_rows, 0.0), axis=1, keepdims=True
            ).astype(jnp.int32)
            next_label.append(label)
            emit = jnp.sum(jnp.where(lane_v == label, logits, 0.0), axis=1, keepdims=True)
            emit = jnp.where(pos < label_len_col, emit - norm, NEG_FILL)
            emit_tb = jnp.zeros((frames, 128), F32)
            for b in range(count):
                emit_tb = jnp.where(lane_b == b, emit[b * frames : (b + 1) * frames, :], emit_tb)
            emit_s[s] = emit_tb

    fill = jnp.full((1, 128), NEG_FILL, F32)
    state = None
    for t in range(frames):
        if t == 0:
            entering = [jnp.zeros((1, 128), F32)] + [fill] * (S - 1)
        else:
            leaving = [state[s] + blank_s[s, t - 1 : t, :] for s in range(S)]
            entering = shifted(leaving, shift_s[t : t + 1, :], -3, fill)
        emits = [emit_s[s, t : t + 1, :] for s in range(S - 1)]
        updated = []
        for s in range(S):
            routes = [
                entering[j] + tree(jnp.add, emits[j:s]) if j < s else entering[j]
                for j in range(s + 1)
            ]
            best = tree(jnp.maximum, routes)
            terms = [jnp.exp(r - best) for r in routes]
            total = tree(jnp.add, terms)
            for j in range(s + 1):
                terms_s[PAIRS.index((j, s)), t : t + 1, :] = terms[j]
            sums_s[s, t : t + 1, :] = total
            updated.append(best + jnp.log(total) if s else best)
        if t == 0:
            state = updated
        else:
            live = t < frame_len_row
            state = [jnp.where(live, n, o) for n, o in zip(updated, state)]

    frame_tb = lax.broadcasted_iota(jnp.int32, (frames, 128), 0)
    ending = frame_tb == frame_len_row - 1
    valid = lax.broadcasted_iota(jnp.int32, (1, 128), 1) < count
    final_start = jnp.sum(jnp.where(ending, start_tb.astype(F32), 0.0), axis=0, keepdims=True)
    final_pos = label_len_row - final_start.astype(jnp.int32)
    share = jnp.where(valid, -1.0 / frame_len_row.astype(F32), 0.0)
    likelihood = jnp.zeros((1, 128), F32)
    grads = []
    for s in range(S):
        here = final_pos == s
        end_blank = jnp.sum(jnp.where(ending, blank_s[s], 0.0), axis=0, keepdims=True)
        likelihood = jnp.where(here, state[s] + end_blank, likelihood)
        grads.append(jnp.where(here, share, 0.0))
        gblank_s[s] = jnp.where(ending & here, share, 0.0)
    loss = jnp.sum(jnp.where(valid, likelihood * share, 0.0), axis=1, keepdims=True)

    for s in range(S):
        inverse = 1.0 / sums_s[s]
        for j in range(s + 1):
            terms_s[PAIRS.index((j, s))] = terms_s[PAIRS.index((j, s))] * inverse

    none = jnp.zeros((1, 128), F32)
    for t in range(frames - 1, 0, -1):
        live = t < frame_len_row
        for s in range(S):
            state_s[s, t : t + 1, :] = jnp.where(live, grads[s], 0.0)
        back = []
        for j in range(S):
            parts = [grads[s] * terms_s[PAIRS.index((j, s)), t : t + 1, :] for s in range(j, S)]
            back.append(tree(jnp.add, parts))
        earlier = shifted(back, -shift_s[t : t + 1, :], -3, none)
        for s in range(S):
            gblank_s[s, t - 1 : t, :] += jnp.where(live, earlier[s], 0.0)
        grads = [jnp.where(live, n, o) for n, o in zip(earlier, grads)]
    for s in range(S):
        state_s[s, 0:1, :] = grads[s]

    def column(table):
        return jnp.concatenate([table[:, b : b + 1] for b in range(count)], axis=0)

    gemit = [jnp.zeros((frames, 128), F32) for _ in range(S - 1)]
    for j, s in PAIRS:
        if j < s:
            flow = state_s[s] * terms_s[PAIRS.index((j, s))]
            for i in range(j, s):
                gemit[i] = gemit[i] + flow
    bias_total = jnp.zeros((1, width), F32)
    for s in range(S):
        pos = start_col + s
        gblank = jnp.where(pos <= label_len_col, column(gblank_s[s]), 0.0)
        if s < S - 1:
            gemit_col = jnp.where(pos < label_len_col, column(gemit[s]), 0.0)
            weight = (gblank + gemit_col) * scale[s]
        else:
            weight = gblank * scale[s]
        grad = jnp.where(lane_v == 0, gblank, 0.0) - scores_s[s] * weight
        if s < S - 1:
            grad = grad + jnp.where(lane_v == next_label[s], gemit_col, 0.0)
        bias_total = bias_total + jnp.sum(grad, axis=0, keepdims=True)
        low_s[s * rows : (s + 1) * rows, :] = grad.astype(BF16)

    grad_enc_proj = jnp.zeros((rows, w_enc_ref.shape[1]), F32)
    grad_pred_proj = jnp.zeros((places, w_pred_ref.shape[1]), F32)
    for s in range(S):
        grad_hidden = jnp.dot(
            low_s[s * rows : (s + 1) * rows, :], w_joint_s[...], preferred_element_type=F32
        )
        active = active_s[s]
        grad_pre = grad_hidden * (1.0 - active * active)
        grad_enc_proj = grad_enc_proj + grad_pre
        grad_pred_proj = grad_pred_proj + over_rows(picks_s[s], grad_pre.astype(BF16))
    bias_s[...] = bias_total
    grad_enc_s[...] = grad_enc_proj.astype(BF16)
    grad_pred_s[...] = grad_pred_proj.astype(BF16)

    core = lax.axis_index("c")
    half = width // 2
    for out_ref, which in ((send_ref, 1 - core), (keep_ref, core)):
        columns = pl.ds(pl.multiple_of(which * half, half), half)
        products = (
            over_rows(enc_ref[...], grad_enc_s[:, columns]),
            over_rows(pred_s[...], grad_pred_s[:, columns]),
            over_rows(low_s[...], hidden_s[:, columns]),
        )
        at = 0
        for product in products:
            for j in range(half // 128):
                out_ref[at : at + width, :] = product[:, j * 128 : (j + 1) * 128]
                at += width
        base = at - (half // 128) * width + vocab
        for j in range(half // 128):
            lanes = pl.ds(pl.multiple_of(which * half + j * 128, 128), 128)
            out_ref[base + j * width : base + j * width + 1, :] = bias_s[:, lanes]
            out_ref[base + j * width + 1 : base + j * width + 2, :] = jnp.broadcast_to(loss, (1, 128))


def local_grads(
    encoder_out, predictor_out, w_encoder, w_predictor, w_joint, joint_bias,
    labels, frame_lens, label_lens, prune_starts,
):
    count, frames, enc_width = encoder_out.shape
    pred_width = predictor_out.shape[2]
    joint_width, vocab = w_joint.shape
    rows = count * frames
    width = -(-vocab // 128) * 128
    places = 128
    vmem = pl.BlockSpec(memory_space=pltpu.VMEM)
    return pl.pallas_call(
        joint_kernel,
        out_shape=(pltpu.VMEM((3 * width * width // 256, 128), F32),) * 2,
        in_specs=[pl.BlockSpec(memory_space=pltpu.HBM)] * 10,
        out_specs=(vmem, vmem),
        scratch_shapes=[
            pltpu.SMEM((count,), jnp.int32),
            pltpu.SMEM((count,), jnp.int32),
            pltpu.VMEM((rows, enc_width), BF16),
            pltpu.VMEM((predictor_out.shape[1], count, pred_width), BF16),
            pltpu.VMEM(w_encoder.shape, BF16),
            pltpu.VMEM(w_predictor.shape, BF16),
            pltpu.VMEM((vocab, joint_width), BF16),
            pltpu.VMEM((1, vocab), F32),
            pltpu.VMEM(labels.shape, jnp.int32),
            pltpu.VMEM(prune_starts.shape, jnp.int32),
            pltpu.SemaphoreType.DMA((10,)),
            pltpu.VMEM((places, pred_width), BF16),
            pltpu.VMEM((width, joint_width), BF16),
            pltpu.VMEM((1, width), F32),
            pltpu.VMEM((S, rows, joint_width), F32),
            pltpu.VMEM((S * rows, joint_width), BF16),
            pltpu.VMEM((S, rows, width), F32),
            pltpu.VMEM((S * rows, width), BF16),
            pltpu.VMEM((S, rows, places), BF16),
            pltpu.VMEM((S, frames, 128), F32),
            pltpu.VMEM((S - 1, frames, 128), F32),
            pltpu.VMEM((frames, 128), jnp.int32),
            pltpu.VMEM((len(PAIRS), frames, 128), F32),
            pltpu.VMEM((S, frames, 128), F32),
            pltpu.VMEM((S, frames, 128), F32),
            pltpu.VMEM((S, frames, 128), F32),
            pltpu.VMEM((rows, joint_width), BF16),
            pltpu.VMEM((places, joint_width), BF16),
        ],
        compiler_params=pltpu.CompilerParams(vmem_limit_bytes=56 * 2**20),
        name="joint",
    )(
        frame_lens, label_lens, encoder_out.reshape(rows, enc_width),
        jnp.swapaxes(predictor_out, 0, 1),        w_encoder, w_predictor, w_joint.T, joint_bias.reshape(1, vocab), labels, prune_starts,
    )


def place_kernel(utterances, sides, *refs):
    half_ref, others = refs[0], refs[1:]
    enc_ref, pred_ref, joint_ref, bias_ref, loss_ref, sems = others[-6:]
    core = lax.axis_index("c")
    width = enc_ref.shape[0]
    vocab = joint_ref.shape[0]
    tiles = width // 256
    outs = (enc_ref, pred_ref, joint_ref)

    def place(h):
        copies = []
        for m, out_ref in enumerate(outs):
            size = out_ref.shape[0]
            for j in range(tiles):
                lane = (h * tiles + j) * 128
                copies.append(
                    pltpu.make_async_copy(
                        half_ref.at[pl.ds((m * tiles + j) * width, size), :],
                        out_ref.at[:, pl.ds(lane, 128)],
                        sems.at[m * tiles + j],
                    )
                )
        for copy in copies:
            copy.start()
        if sides:
            bias_ref[...] = others[3][...]
        for j in range(tiles):
            at = (2 * tiles + j) * width + vocab
            lane = (h * tiles + j) * 128
            size = min(128, vocab - lane)
            bias_ref[:, lane : lane + size] = half_ref[at : at + 1, :size]
        at = 2 * tiles * width + vocab + 1
        loss_ref[...] = half_ref[at : at + 1, 0:1] / utterances
        for copy in copies:
            copy.wait()

    for h in range(2):
        @pl.when((core + sides) % 2 == h)
        def _():
            place(h)


def place(half, so_far, utterances, shapes):
    vmem = pl.BlockSpec(memory_space=pltpu.VMEM)
    hbm = pl.BlockSpec(memory_space=pltpu.HBM)
    big, small = shapes[:3], shapes[3:]
    out_shape = [pltpu.HBM(d, F32) for d in big] + [jax.ShapeDtypeStruct(d, F32) for d in small]
    inputs = (half, *so_far[:4])
    return pl.pallas_call(
        functools.partial(place_kernel, utterances, int(bool(so_far))),
        out_shape=out_shape,
        in_specs=[vmem] + ([hbm] * 3 + [vmem] if so_far else []),
        out_specs=[hbm] * 3 + [vmem] * 2,
        scratch_shapes=[pltpu.SemaphoreType.DMA((6,))],
        input_output_aliases={1: 0, 2: 1, 3: 2} if so_far else {},
        compiler_params=pltpu.CompilerParams(vmem_limit_bytes=8 * 2**20),
        cost_estimate=pl.CostEstimate(
            flops=2**24, bytes_accessed=2 * half.size * 4, transcendentals=0
        ),
        name="place",
    )(*inputs)


def merge_kernel(keep_ref, recv_ref, out_ref):
    out_ref[...] = keep_ref[...] + recv_ref[...]

    @pl.when(lax.axis_index("c") == SECOND)
    def _():
        spare = out_ref.shape[0] - 8
        first = out_ref[spare:, :]
        out_ref[spare:, :] = lax.fori_loop(0, STAGGER, lambda _, v: jnp.tanh(v), first)


def merge(keep, recv):
    vmem = pl.BlockSpec(memory_space=pltpu.VMEM)
    return pl.pallas_call(
        merge_kernel,
        out_shape=pltpu.VMEM(keep.shape, F32),
        in_specs=[vmem, vmem],
        out_specs=vmem,
        input_output_aliases={0: 0},
        compiler_params=pltpu.CompilerParams(vmem_limit_bytes=8 * 2**20),
        name="merge",
    )(keep, recv)


def swap_cores(value):
    return lax.ppermute(value, "c", [(0, 1), (1, 0)])


def sum_at_owner(value, axes):
    members = lax.axis_size(axes)
    arrived = lax.all_to_all(value, axes, split_axis=0, concat_axis=0, tiled=True)
    return arrived.reshape(members, -1, value.shape[1]).sum(axis=0)


def from_all(value, axes):
    members = lax.axis_size(axes)
    spread = jnp.broadcast_to(value[None], (members, *value.shape))
    spread = spread.reshape(-1, value.shape[1])
    return lax.all_to_all(spread, axes, split_axis=0, concat_axis=0, tiled=True)


def sum_everywhere(value, axes):
    sizes = [lax.axis_size(a) for a in axes]
    assert sizes == [2, 2]
    arrived = []
    for step in (2, 1, 3):
        pairs = [
            (2 * (n % 2) + n // 2, 2 * ((n + step) % 4 % 2) + (n + step) % 4 // 2)
            for n in range(4)
        ]
        arrived.append(lax.ppermute(value, axes, pairs))
    return (value + arrived[0]) + (arrived[1] + arrived[2])


def shards(*args):
    keep, send = local_grads(*args)
    mine = merge(keep, swap_cores(send))
    mine = sum_at_owner(mine, NEAR)
    mine = sum_everywhere(mine, FAR)
    mine = from_all(mine, NEAR)
    other = swap_cores(mine)
    width, vocab = args[4].shape
    utterances = args[0].shape[0] * lax.axis_size(AXES)
    shapes = ((width, width), (width, width), (vocab, width), (1, vocab), (1, 1))
    so_far = place(mine, (), utterances, shapes)
    grad_encoder, grad_predictor, grad_joint, grad_bias, loss = place(
        other, so_far, utterances, shapes
    )
    return grad_encoder, grad_predictor, grad_joint.T, grad_bias.reshape(vocab), loss.reshape(())


def solution(mesh):
    mesh = jax.sharding.Mesh(mesh.devices.reshape(2, 2, 4, 4, 2, 2), AXES)
    in_specs = (
        P(AXES, None, None), P(AXES, None, None), P(), P(), P(), P(),
        P(AXES, None), P(AXES), P(AXES), P(AXES, None),
    )
    return jax.shard_map(
        shards, mesh=mesh, in_specs=in_specs, out_specs=(P(),) * 5, check_vma=False
    )
```
